32 devices in a mesh: seq: 8 (over z, y), head: 4 (over x, core).
Axes of the slice: x: 2, y: 2, z: 4, core: 2. Of those that a mesh axis runs over, the one named last changes fastest.
Arguments:
- queries: bfloat16 [4096, 4096], P('seq', 'head'), may hold values from -5 to 5
- keys: bfloat16 [4096, 1024], P('seq', 'head'), may hold values from -5 to 5
- values: bfloat16 [4096, 1024], P('seq', 'head'), may hold values from -5 to 5
- doc_lengths: int32 [16], replicated, may hold values from 1 to 2048, 4096 in all
- out_weight: bfloat16 [4096, 4096], P('head', 'seq'), may hold values from -0.125 to 0.125
Outputs:
- mixed: bfloat16 [4096, 4096], P('seq', 'head')
The draws below stay inside these ranges and needn't reach their ends.
Inputs may be any that keep to these rules, and one draw needn't show every extreme that they name: `doc_lengths`: the lengths sum to 4096, and one document is exactly 2048 tokens long.
All inputs are finite; a program needn't handle non-finite values.
Results may differ from the reference program's by a relative error of at most 0.012.
Values may be sent and summed in bfloat16 or wider, within the bound.
A program may use at most 128 MiB of HBM per device.

```python
import math
import jax
import jax.numpy as jnp
import numpy as np
from jax import lax

D = 4096
HQ = 32
KV = 8
DH = 128
TOK_DEV = 512
TOKENS = 4096
MOST = 2048
DOCS = 16


def draw_keys(key, part):
    base = jnp.clip(jax.random.normal(jax.random.fold_in(key, 1), (TOKENS, KV * DH), jnp.float32), -5.0, 5.0)
    return base.astype(jnp.bfloat16)


def draw_queries(key, part):
    base = jnp.clip(jax.random.normal(jax.random.fold_in(key, 2), (TOKENS, HQ * DH), jnp.float32), -5.0, 5.0)
    return base.astype(jnp.bfloat16)


def raised(array, key, source, target, parts, factor):
    def block_of(axis_at):
        return (jnp.arange(array.shape[axis_at]) // (array.shape[axis_at] // parts)).reshape((-1,) + (1,) * (array.ndim - 1 - axis_at))

    one_side = jax.random.permutation(key, parts)[block_of(target)]
    other_side = (block_of(target) + parts // 2) % parts
    return jnp.where((block_of(source) == one_side) | (block_of(source) == other_side), factor * array, array)


def steps_of(key, dims, cuts, low, high):
    gain, own = 1.0, jax.random.fold_in(key, 6)
    for axis_at, parts in cuts:
        heights = jnp.exp(jax.random.uniform(jax.random.fold_in(own, axis_at), (parts,), jnp.float32, low / len(cuts), high / len(cuts)))
        gain = gain * jnp.repeat(heights, dims[axis_at] // parts).reshape([-1 if axis == axis_at else 1 for axis in range(len(dims))])
    return gain


def length_profile(amount, total, most, slope):
    loads = [(1 << 20) // math.isqrt(grade ** slope) + 1 for grade in range(2, amount + 1)]
    rest, given = total - most - (amount - 1), [1] * (amount - 1)
    while rest > 0:
        free = [i for i in range(amount - 1) if given[i] < most]
        mass, left = sum([loads[i] for i in free]), rest
        for i in free:
            addition = min(most - given[i], max(1, left * loads[i] // mass), rest)
            given[i] = given[i] + addition
            rest = rest - addition
    return np.array([most] + given)


def uneven(stream_key, count, total, limit, slope):
    if count == 2:
        one = jax.random.randint(stream_key, (), max(1, total - limit), min(limit, total - 1) + 1)
        return jnp.stack([one, total - one])
    sizes = jnp.asarray(length_profile(count, total, limit, slope), jnp.int32)
    twos = (count - 1) // 2
    source_of, taker = sizes[1:1 + 2 * twos:2], sizes[2:2 + 2 * twos:2]
    margin = jnp.minimum(source_of - 1, limit - taker)
    passed = jax.random.randint(jax.random.fold_in(stream_key, 1), (twos,), 0, 1 << 20) % (margin + 1)
    sizes = sizes.at[1:1 + 2 * twos:2].set(source_of - passed).at[2:2 + 2 * twos:2].set(taker + passed)
    return sizes[jax.random.permutation(jax.random.fold_in(stream_key, 2), count)]


def normal_values(rng, dims, deviation, limit, split=(), kind=jnp.bfloat16):
    array = jax.random.normal(rng, dims, jnp.float32) * deviation
    if len(split) > 0:
        array = steps_of(rng, dims, split, -0.22, 0.18) * array
    return jnp.clip(array, min=-limit, max=limit).astype(kind)


def heavy_noise(stream_key, dims, width, bound, shards, heavy, held_as=jnp.bfloat16):
    entries = width * jax.random.normal(stream_key, dims, jnp.float32)
    if shards:
        entries = entries * steps_of(stream_key, dims, shards, -0.22, 0.18)
    return jnp.clip(raised(entries, jax.random.fold_in(stream_key, 3), *heavy), -bound, bound).astype(held_as)


def setup_inputs(seed: int = 0) -> dict:
    seeds = jax.random.split(jax.random.key(seed), 6)
    return {
        "queries": draw_queries(jax.random.fold_in(seeds[5], 71), 0),
        "keys": draw_keys(jax.random.fold_in(seeds[5], 71), 0),
        "values": normal_values(seeds[2], (TOKENS, KV * DH), 1.0, 5.0, ((0, 8), (1, 4))),
        "doc_lengths": uneven(seeds[3], DOCS, TOKENS, MOST, 2).astype(jnp.int32),
        "out_weight": heavy_noise(seeds[4], (HQ * DH, D), (HQ * DH) ** -0.5, 0.125, ((0, 4), (1, 8)), (0, 1, 8, 2.0)),
    }


def doc_index(positions, starts):
    return jnp.sum((starts[None, :] <= positions[:, None]).astype(jnp.int32), axis=1) - 1


def reference(queries, keys, values, doc_lengths, out_weight):
    starts = (jnp.cumsum(doc_lengths) - doc_lengths).astype(jnp.int32)
    total_rows = queries.shape[0]
    group_size = HQ // KV
    window = MOST + TOK_DEV
    num_blocks = total_rows // TOK_DEV
    temper = DH ** -0.5

    def attend_block(flat_index):
        q_block = flat_index // KV
        kv_head = flat_index % KV
        q_first = (q_block * TOK_DEV).astype(jnp.int32)
        k_first = jnp.clip(q_first - MOST, 0, total_rows - window).astype(jnp.int32)
        q_rows = lax.dynamic_slice(queries, (q_first, (kv_head * group_size * DH).astype(jnp.int32)), (TOK_DEV, group_size * DH))
        q_rows = q_rows.astype(jnp.float32).reshape(TOK_DEV, group_size, DH)
        k_rows = lax.dynamic_slice(keys, (k_first, (kv_head * DH).astype(jnp.int32)), (window, DH)).astype(jnp.float32)
        v_rows = lax.dynamic_slice(values, (k_first, (kv_head * DH).astype(jnp.int32)), (window, DH)).astype(jnp.float32)
        scores = jnp.einsum("qgd,nd->gqn", q_rows, k_rows) * temper
        q_pos = q_first + jnp.arange(TOK_DEV, dtype=jnp.int32)
        k_pos = k_first + jnp.arange(window, dtype=jnp.int32)
        q_doc = doc_index(q_pos, starts)
        k_doc = doc_index(k_pos, starts)
        allowed = (k_doc[None, :] == q_doc[:, None]) & (k_pos[None, :] <= q_pos[:, None])
        scores = jnp.where(allowed[None], scores, jnp.float32(-1e30))
        row_max = jnp.max(scores, axis=-1, keepdims=True)
        probs = jnp.where(allowed[None], jnp.exp(scores - row_max), jnp.float32(0.0))
        row_sum = jnp.sum(probs, axis=-1)
        weights = probs.astype(jnp.bfloat16)
        result = jnp.einsum("gqn,nd->gqd", weights.astype(jnp.float32), v_rows) / row_sum[..., None]
        return jnp.transpose(result, (1, 0, 2)).reshape(TOK_DEV, group_size * DH).astype(jnp.bfloat16)

    blocks = lax.map(attend_block, jnp.arange(num_blocks * KV, dtype=jnp.int32))
    attn = blocks.reshape(num_blocks, KV, TOK_DEV, group_size * DH)
    attn = jnp.transpose(attn, (0, 2, 1, 3)).reshape(total_rows, HQ * DH)
    return jnp.dot(attn, out_weight, preferred_element_type=jnp.float32).astype(jnp.bfloat16)
```

```python
import functools
import math

import jax
import jax.numpy as jnp
from jax import lax
from jax.experimental import pallas as pl
from jax.experimental.pallas import tpu as pltpu
from jax.sharding import PartitionSpec as P

HQ = 32
KV = 8
DH = 128
MOST = 2048
CHUNKS = 4
PIECE = 128
MESH = pl.DeviceIdType.MESH


def kernel(
    n_seq, lens_ref, q_ref, k_hbm, v_hbm, w_hbm, out_ref,
    kbuf, vbuf, wbuf, bias, vt, mx, sm, acc, both,
    tmp, keep, sum1, sum2, give3, got3,
    load_sem, kvz_send, kvy_send, kv_recv, wl_send, wl_recv, wr_send, wr_recv,
    at_send, at_recv, s1_send, s1_recv, s2_send, s2_recv, s3_send, s3_recv,
):
    s, h = lax.axis_index("seq"), lax.axis_index("head")
    pairs = n_seq // 2
    p, m = s // 2, lax.rem(s, 2)
    mate = s + 1 - 2 * m
    right = lax.rem(p + 1, pairs) * 2 + m
    left = lax.rem(p + pairs - 1, pairs) * 2 + m
    near = h + 1 - 2 * lax.rem(h, 2)
    far = lax.rem(h + 2, 4)
    rows = q_ref.shape[0]
    depth, wc = w_hbm.shape
    pieces, wcp = wbuf.shape[1], wbuf.shape[3]
    half = depth // 2
    groups = pairs // 4
    group_size = HQ // KV
    part = rows * 2 // CHUNKS
    has_up, has_down = p + 1 < pairs, p >= 1
    scale = DH ** (-0.5) * math.log2(math.e)

    def copy(src, dst, send, recv, seq, head):
        return pltpu.make_async_remote_copy(
            src_ref=src, dst_ref=dst, send_sem=send, recv_sem=recv,
            device_id={"seq": seq, "head": head}, device_id_type=MESH,
        )

    def kv_copies(src_slot, dst_slot, j, send, target):
        cols = pl.ds(pl.multiple_of(j * DH, DH), DH)
        return [
            copy(buf.at[src_slot, :, cols], buf.at[dst_slot, :, cols],
                 send.at[j, c], kv_recv.at[dst_slot, j, c], target, h)
            for c, buf in enumerate((kbuf, vbuf))
        ]

    def w_copy(block, c, step, send, recv, target):
        piece = wbuf.at[block, c]
        return copy(piece, piece, send.at[step, c], recv.at[step, c], target, h)

    def left_copy(step, c):
        return w_copy(jnp.minimum(p + step, pairs - 1), c, step, wl_send, wl_recv, left)

    def right_copy(step, c):
        return w_copy(jnp.maximum(p - step, 0), c, step, wr_send, wr_recv, right)

    loads = [
        pltpu.make_async_copy(k_hbm, kbuf.at[0], load_sem.at[0]),
        pltpu.make_async_copy(v_hbm, vbuf.at[0], load_sem.at[1]),
    ] + [
        pltpu.make_async_copy(w_hbm.at[:, c * wcp:(c + 1) * wcp], wbuf.at[p, c], load_sem.at[2 + c])
        for c in range(pieces)
    ]
    for load in loads:
        load.start()

    barrier = pltpu.get_barrier_semaphore()
    for seq, head in ((mate, h), (left, h), (right, h), (s, near), (s, far)):
        pl.semaphore_signal(barrier, inc=1, device_id={"seq": seq, "head": head}, device_id_type=MESH)
    pl.semaphore_wait(barrier, 5)

    loads[0].wait()
    loads[1].wait()
    has_next = s + 2 < n_seq
    for j in range(2):
        @pl.when(has_next)
        def _():
            for c in kv_copies(0, 2, j, kvz_send.at[0], right):
                c.start()

        @pl.when(m == 0)
        def _():
            for c in kv_copies(0, 1, j, kvy_send.at[0], mate):
                c.start()

    for load in loads[2:]:
        load.wait()

    @pl.when(has_down)
    def _():
        for c in range(pieces):
            left_copy(0, c).start()

    q_pos = s * rows + lax.broadcasted_iota(jnp.int32, (1, rows), 1)
    start = jnp.int32(0)
    first = jnp.zeros((1, rows), jnp.int32)
    for d in range(1, lens_ref.shape[0]):
        start = start + lens_ref[d - 1]
        first = jnp.where(q_pos >= start, start, first)

    def attn_copy(j):
        return copy(both.at[1, j], both.at[0, j], at_send.at[j], at_recv.at[j], mate, h)

    def finish(j):
        def one(g, _):
            i = j * group_size + g
            full = jnp.transpose(acc[i] / sm[i])
            both[1, j, :, pl.ds(pl.multiple_of(g * DH, DH), DH)] = full.astype(jnp.bfloat16)
            return 0

        lax.fori_loop(0, group_size, one, 0)
        attn_copy(j).start()

    def take_left(t, c):
        left_copy(t, c).wait_recv()

        @pl.when(has_down)
        def _():
            left_copy(t + 1, c).start()

    def take_right(t, c):
        right_copy(t, c).wait_recv()

        @pl.when(has_up)
        def _():
            right_copy(t + 1, c).start()

    def step(i, _):
        k = jnp.maximum(i - 2, 0)
        w = lax.rem(k, 4)
        slot = jnp.where(i < 2, 0, 2 + 2 * (k // 4) - lax.rem(w, 2))
        j = jnp.where(i < 2, i, w // 2)

        @pl.when((i >= 2) & (s >= slot))
        def _():
            for c in kv_copies(slot, slot, j, kvz_send.at[0], right):
                c.wait_recv()

            @pl.when((slot == 2) & has_next)
            def _():
                for c in kv_copies(2, 4, j, kvz_send.at[1], right):
                    c.start()

            @pl.when(slot == 2)
            def _():
                for c in kv_copies(2, 3 - 2 * m, j, kvy_send.at[1], mate):
                    c.start()

            @pl.when((slot == 4) & (m == 1))
            def _():
                for c in kv_copies(4, 3, j, kvy_send.at[2], mate):
                    c.start()

        @pl.when((i == 4) & has_up)
        def _():
            for c in range(pieces):
                right_copy(0, c).start()

        for c in range(pieces):
            @pl.when((i == 11 - 2 * (pieces - c)) & has_up)
            def _():
                take_left(0, c)

        @pl.when(s >= slot)
        def _():
            cols = pl.ds(pl.multiple_of(j * DH, DH), DH)
            k_pos = (s - slot) * rows + lax.broadcasted_iota(jnp.int32, (rows, rows), 0)
            bias[...] = jnp.where((k_pos >= first) & (k_pos <= q_pos), 0.0, -1e30)
            vt[...] = jnp.transpose(vbuf[slot, :, cols])

            def one(g, _):
                at = j * group_size + g
                q = q_ref[:, pl.ds(pl.multiple_of(at * DH, DH), DH)]
                scores = lax.dot_general(
                    kbuf[slot, :, cols], q, (((1,), (1,)), ((), ())),
                    preferred_element_type=jnp.float32,
                ) * scale + bias[...]
                top = jnp.max(scores, axis=0, keepdims=True)
                old = jnp.where(i < 2, jnp.full_like(top, -1e30), mx[at])
                new = jnp.maximum(old, top)
                probs = jnp.exp2(scores - new)
                fade = jnp.exp2(old - new)
                mx[at] = new
                total = jnp.sum(probs, axis=0, keepdims=True)
                sm[at] = jnp.where(i < 2, total, sm[at] * fade + total)
                mixed = jnp.dot(vt[...], probs.astype(jnp.bfloat16), preferred_element_type=jnp.float32)

                @pl.when(i < 2)
                def _():
                    acc[at] = mixed

                @pl.when(i >= 2)
                def _():
                    acc[at] = acc[at] * fade + mixed

                return 0

            lax.fori_loop(0, group_size, one, 0)

        for at, jj in ((7, 0), (9, 1)):
            @pl.when(i == at)
            def _():
                finish(jj)

        return 0

    lax.fori_loop(0, 10, step, 0)

    for j in range(2):
        attn_copy(j).wait_recv()

    per_side = CHUNKS // 2

    def first_copy(b, c, r):
        return copy(sum1.at[b, c, r], sum1.at[b, c, r], s1_send.at[b, c, r], s1_recv.at[b, c, r], s, near)

    def second_copy(b, c, r):
        return copy(sum2.at[b, c, r], sum2.at[b, c, r], s2_send.at[b, c, r], s2_recv.at[b, c, r], s, far)

    def third_copy(g, c, r):
        return copy(give3.at[g, c, r], got3.at[g, c, r], s3_send.at[g, c, r], s3_recv.at[g, c, r], mate, h)

    def odd(b):
        return lax.rem(b // groups + h, 2) == 1

    def piece_step(b, c):
        away = odd(b)

        def chunk(r, _):
            side = r // per_side
            at = pl.multiple_of(lax.rem(r, per_side) * part, part)
            y = (jnp.dot(both[side, 0, pl.ds(at, part), :], wbuf[b, c, :half, :],
                         preferred_element_type=jnp.float32)
                 + jnp.dot(both[side, 1, pl.ds(at, part), :], wbuf[b, c, half:, :],
                           preferred_element_type=jnp.float32))

            @pl.when(away)
            def _():
                sum1[b, c, r] = y.astype(jnp.bfloat16)
                first_copy(b, c, r).start()

            @pl.when(jnp.logical_not(away))
            def _():
                tmp[r] = y

            return 0

        lax.fori_loop(0, CHUNKS, chunk, 0)

        @pl.when(jnp.logical_not(away))
        def _():
            home = b // groups == h
            g = lax.rem(b, groups)

            def settle(r, _):
                first_copy(b, c, r).wait_recv()
                y = tmp[r] + sum1[b, c, r].astype(jnp.float32)

                @pl.when(home)
                def _():
                    keep[g, c, r] = y

                @pl.when(jnp.logical_not(home))
                def _():
                    sum2[b, c, r] = y.astype(jnp.bfloat16)
                    second_copy(b, c, r).start()

                return 0

            lax.fori_loop(0, CHUNKS, settle, 0)

    def block_step(e, _):
        d = (e + 1) // 2
        from_up = lax.rem(e, 2) == 1
        b = jnp.where(from_up, p + d, p - d)
        exists = (b >= 0) & (b < pairs)
        b = jnp.clip(b, 0, pairs - 1)

        @pl.when(exists)
        def _():
            def one(c, _):
                @pl.when((e >= 4) & from_up)
                def _():
                    take_left(d - 1, c)

                @pl.when((e >= 4) & jnp.logical_not(from_up))
                def _():
                    take_right(d - 1, c)

                piece_step(b, c)
                return 0

            lax.fori_loop(0, pieces, one, 0)

        @pl.when((e == 0) & has_down)
        def _():
            for c in range(pieces):
                take_right(0, c)

        @pl.when((e == 1) & (p + 2 < pairs))
        def _():
            for c in range(pieces):
                take_left(1, c)

        return 0

    lax.fori_loop(0, 2 * pairs - 1, block_step, 0)

    def result(g, c, r):
        b = h * groups + g
        second_copy(b, c, r).wait_recv()
        return (keep[g, c, r] + sum2[b, c, r].astype(jnp.float32)).astype(jnp.bfloat16)

    def place(g, c, r, member, value):
        at = pl.multiple_of(lax.rem(r, per_side) * part, part)
        first_col = pl.multiple_of((2 * g + member) * wc + c * wcp, wcp)
        out_ref[pl.ds(at, part), pl.ds(first_col, wcp)] = value

    for g in range(groups):
        def pass_on(c, _):
            for r in range(per_side):
                give3[g, c, r] = result(g, c, r)
                third_copy(g, c, r).start()
            for r in range(per_side, CHUNKS):
                place(g, c, r, m, result(g, c, r))
            return 0

        lax.fori_loop(0, pieces, pass_on, 0)

    for g in range(groups):
        def take_in(c, _):
            for r in range(per_side):
                third_copy(g, c, r).wait_recv()
                place(g, c, r, 1 - m, got3[g, c, r])
            return 0

        lax.fori_loop(0, pieces, take_in, 0)

    for j in range(2):
        @pl.when(has_next)
        def _():
            for c in kv_copies(0, 2, j, kvz_send.at[0], right):
                c.wait_send()

        @pl.when((s >= 2) & has_next)
        def _():
            for c in kv_copies(2, 4, j, kvz_send.at[1], right):
                c.wait_send()

        @pl.when(m == 0)
        def _():
            for c in kv_copies(0, 1, j, kvy_send.at[0], mate):
                c.wait_send()

        @pl.when(s >= 2)
        def _():
            for c in kv_copies(2, 3 - 2 * m, j, kvy_send.at[1], mate):
                c.wait_send()

        @pl.when((s >= 4) & (m == 1))
        def _():
            for c in kv_copies(4, 3, j, kvy_send.at[2], mate):
                c.wait_send()

        attn_copy(j).wait_send()

    def drain(b, _):
        def one(c, _):
            @pl.when(has_down & (p + b < pairs))
            def _():
                left_copy(b, c).wait_send()

            @pl.when(has_up & (p - b >= 0))
            def _():
                right_copy(b, c).wait_send()

            for r in range(CHUNKS):
                @pl.when(odd(b))
                def _():
                    first_copy(b, c, r).wait_send()

                @pl.when(jnp.logical_not(odd(b)) & (b // groups != h))
                def _():
                    second_copy(b, c, r).wait_send()

            return 0

        return lax.fori_loop(0, pieces, one, 0)

    lax.fori_loop(0, pairs, drain, 0)
    for g in range(groups):
        def sent(c, _):
            for r in range(per_side):
                third_copy(g, c, r).wait_send()
            return 0

        lax.fori_loop(0, pieces, sent, 0)


def body(n_seq, queries, keys, values, doc_lengths, out_weight):
    rows, width = queries.shape
    kv_width = keys.shape[1]
    depth, wc = out_weight.shape
    pairs = n_seq // 2
    groups = pairs // 4
    heads = width // DH
    part = rows * 2 // CHUNKS
    wcp = min(PIECE, wc)
    pieces = wc // wcp
    slots = -(-(MOST - 1) // rows) + 1
    vmem = pl.BlockSpec(memory_space=pltpu.VMEM)
    hbm = pl.BlockSpec(memory_space=pl.ANY)
    bf, f32, dma = jnp.bfloat16, jnp.float32, pltpu.SemaphoreType.DMA
    return pl.pallas_call(
        functools.partial(kernel, n_seq),
        out_shape=jax.ShapeDtypeStruct((rows, wc * 2 * (pairs // 4)), bf),
        in_specs=[pl.BlockSpec(memory_space=pltpu.SMEM), vmem, hbm, hbm, hbm],
        out_specs=vmem,
        scratch_shapes=[
            pltpu.VMEM((slots, rows, kv_width), bf),
            pltpu.VMEM((slots, rows, kv_width), bf),
            pltpu.VMEM((pairs, pieces, depth, wcp), bf),
            pltpu.VMEM((rows, rows), f32),
            pltpu.VMEM((DH, rows), bf),
            pltpu.VMEM((heads, 1, rows), f32),
            pltpu.VMEM((heads, 1, rows), f32),
            pltpu.VMEM((heads, DH, rows), f32),
            pltpu.VMEM((2, 2, rows, width // 2), bf),
            pltpu.VMEM((CHUNKS, part, wcp), f32),
            pltpu.VMEM((groups, pieces, CHUNKS, part, wcp), f32),
            pltpu.VMEM((pairs, pieces, CHUNKS, part, wcp), bf),
            pltpu.VMEM((pairs, pieces, CHUNKS, part, wcp), bf),
            pltpu.VMEM((groups, pieces, CHUNKS // 2, part, wcp), bf),
            pltpu.VMEM((groups, pieces, CHUNKS // 2, part, wcp), bf),
            dma((2 + pieces,)), dma((2, 2, 2)), dma((3, 2, 2)), dma((slots, 2, 2)),
            dma((pairs, pieces)), dma((pairs, pieces)), dma((pairs, pieces)), dma((pairs, pieces)),
            dma((2,)), dma((2,)),
            dma((pairs, pieces, CHUNKS)), dma((pairs, pieces, CHUNKS)),
            dma((pairs, pieces, CHUNKS)), dma((pairs, pieces, CHUNKS)),
            dma((groups, pieces, CHUNKS // 2)), dma((groups, pieces, CHUNKS // 2)),
        ],
        compiler_params=pltpu.CompilerParams(
            collective_id=0, has_side_effects=True, vmem_limit_bytes=56 * 1024 * 1024
        ),
    )(doc_lengths, queries, keys, values, out_weight)


def solution(mesh):
    return jax.shard_map(
        functools.partial(body, mesh.shape["seq"]),
        mesh=mesh,
        in_specs=(P("seq", "head"), P("seq", "head"), P("seq", "head"), P(), P("head", "seq")),
        out_specs=P("seq", "head"),
        check_vma=False,
    )
```

```python
import functools
import math

import jax
import jax.numpy as jnp
from jax import lax
from jax.experimental import pallas as pl
from jax.experimental.pallas import tpu as pltpu
from jax.sharding import PartitionSpec as P

HQ = 32
KV = 8
DH = 128
MOST = 2048
CHUNKS = 4
PIECE = 128
MESH = pl.DeviceIdType.MESH


def kernel(
    n_seq, lens_ref, q_ref, k_hbm, v_hbm, w_hbm, out_ref,
    kbuf, vbuf, wbuf, bias, vt, mx, sm, acc, both,
    tmp, keep, sum1, sum2, give3, got3, lent, lsum1, lsum2, lgot,
    load_sem, kvz_send, kvy_send, kv_recv, wl_send, wl_recv, wr_send, wr_recv,
    at_send, at_recv, s1_send, s1_recv, s2_send, s2_recv, s3_send, s3_recv,
    la_send, la_recv, l1_send, l1_recv, l2_send, l2_recv,
):
    s, h = lax.axis_index("seq"), lax.axis_index("head")
    pairs = n_seq // 2
    p, m = s // 2, lax.rem(s, 2)
    mate = s + 1 - 2 * m
    right = lax.rem(p + 1, pairs) * 2 + m
    left = lax.rem(p + pairs - 1, pairs) * 2 + m
    near = h + 1 - 2 * lax.rem(h, 2)
    far = lax.rem(h + 2, 4)
    rows = q_ref.shape[0]
    depth, wc = w_hbm.shape
    pieces, wcp = wbuf.shape[1], wbuf.shape[3]
    half = depth // 2
    groups = pairs // 4
    group_size = HQ // KV
    part = rows * 2 // CHUNKS
    wide = 2 if pieces % 2 == 0 else 1
    has_up, has_down = p + 1 < pairs, p >= 1
    is_last, is_helper = p == pairs - 1, p == pairs - 2
    scale = DH ** (-0.5) * math.log2(math.e)

    def copy(src, dst, send, recv, seq, head):
        return pltpu.make_async_remote_copy(
            src_ref=src, dst_ref=dst, send_sem=send, recv_sem=recv,
            device_id={"seq": seq, "head": head}, device_id_type=MESH,
        )

    def kv_copies(src_slot, dst_slot, j, send, target):
        cols = pl.ds(pl.multiple_of(j * DH, DH), DH)
        return [
            copy(buf.at[src_slot, :, cols], buf.at[dst_slot, :, cols],
                 send.at[j, c], kv_recv.at[dst_slot, j, c], target, h)
            for c, buf in enumerate((kbuf, vbuf))
        ]

    def w_copy(block, c, step, send, recv, target):
        piece = wbuf.at[block, c]
        return copy(piece, piece, send.at[step, c], recv.at[step, c], target, h)

    def left_copy(step, c):
        return w_copy(jnp.minimum(p + step, pairs - 1), c, step, wl_send, wl_recv, left)

    def right_copy(step, c):
        return w_copy(jnp.maximum(p - step, 0), c, step, wr_send, wr_recv, right)

    loads = [
        pltpu.make_async_copy(k_hbm, kbuf.at[0], load_sem.at[0]),
        pltpu.make_async_copy(v_hbm, vbuf.at[0], load_sem.at[1]),
    ] + [
        pltpu.make_async_copy(w_hbm.at[:, c * wcp:(c + 1) * wcp], wbuf.at[p, c], load_sem.at[2 + c])
        for c in range(pieces)
    ]
    for load in loads:
        load.start()

    barrier = pltpu.get_barrier_semaphore()
    for seq, head in ((mate, h), (left, h), (right, h), (s, near), (s, far)):
        pl.semaphore_signal(barrier, inc=1, device_id={"seq": seq, "head": head}, device_id_type=MESH)
    pl.semaphore_wait(barrier, 5)

    loads[0].wait()
    loads[1].wait()
    has_next = s + 2 < n_seq
    for j in range(2):
        @pl.when(has_next)
        def _():
            for c in kv_copies(0, 2, j, kvz_send.at[0], right):
                c.start()

        @pl.when(m == 0)
        def _():
            for c in kv_copies(0, 1, j, kvy_send.at[0], mate):
                c.start()

    for load in loads[2:]:
        load.wait()

    @pl.when(has_down)
    def _():
        for c in range(pieces):
            left_copy(0, c).start()

    q_pos = s * rows + lax.broadcasted_iota(jnp.int32, (1, rows), 1)
    start = jnp.int32(0)
    first = jnp.zeros((1, rows), jnp.int32)
    for d in range(1, lens_ref.shape[0]):
        start = start + lens_ref[d - 1]
        first = jnp.where(q_pos >= start, start, first)

    def attn_copy(j):
        return copy(both.at[1, j], both.at[0, j], at_send.at[j], at_recv.at[j], mate, h)

    def lend_own(j):
        return copy(both.at[1, j], lent.at[1, j], la_send.at[0, j], la_recv.at[0, j], left, h)

    def lend_other(j, source, target):
        return copy(source, lent.at[0, j], la_send.at[1, j], la_recv.at[1, j], target, h)

    def finish(j):
        def one(g, _):
            i = j * group_size + g
            full = jnp.transpose(acc[i] / sm[i])
            both[1, j, :, pl.ds(pl.multiple_of(g * DH, DH), DH)] = full.astype(jnp.bfloat16)
            return 0

        lax.fori_loop(0, group_size, one, 0)
        attn_copy(j).start()

        @pl.when(is_last)
        def _():
            lend_own(j).start()

    def take_left(t, c):
        left_copy(t, c).wait_recv()

        @pl.when(has_down)
        def _():
            left_copy(t + 1, c).start()

    def take_right(t, c):
        right_copy(t, c).wait_recv()

        @pl.when(has_up & jnp.logical_not(is_helper & (p == t + 1)))
        def _():
            right_copy(t + 1, c).start()

    def step(i, _):
        k = jnp.maximum(i - 2, 0)
        w = lax.rem(k, 4)
        slot = jnp.where(i < 2, 0, 2 + 2 * (k // 4) - lax.rem(w, 2))
        j = jnp.where(i < 2, i, w // 2)

        @pl.when((i >= 2) & (s >= slot))
        def _():
            for c in kv_copies(slot, slot, j, kvz_send.at[0], right):
                c.wait_recv()

            @pl.when((slot == 2) & has_next)
            def _():
                for c in kv_copies(2, 4, j, kvz_send.at[1], right):
                    c.start()

            @pl.when(slot == 2)
            def _():
                for c in kv_copies(2, 3 - 2 * m, j, kvy_send.at[1], mate):
                    c.start()

            @pl.when((slot == 4) & (m == 1))
            def _():
                for c in kv_copies(4, 3, j, kvy_send.at[2], mate):
                    c.start()

        @pl.when((i == 4) & has_up)
        def _():
            for c in range(pieces):
                right_copy(0, c).start()

        for c in range(pieces):
            @pl.when((i == 11 - 2 * (pieces - c)) & has_up)
            def _():
                take_left(0, c)

        @pl.when(s >= slot)
        def _():
            cols = pl.ds(pl.multiple_of(j * DH, DH), DH)
            k_pos = (s - slot) * rows + lax.broadcasted_iota(jnp.int32, (rows, rows), 0)
            bias[...] = jnp.where((k_pos >= first) & (k_pos <= q_pos), 0.0, -1e30)
            vt[...] = jnp.transpose(vbuf[slot, :, cols])

            def one(g, _):
                at = j * group_size + g
                q = q_ref[:, pl.ds(pl.multiple_of(at * DH, DH), DH)]
                scores = lax.dot_general(
                    kbuf[slot, :, cols], q, (((1,), (1,)), ((), ())),
                    preferred_element_type=jnp.float32,
                ) * scale + bias[...]
                top = jnp.max(scores, axis=0, keepdims=True)
                old = jnp.where(i < 2, jnp.full_like(top, -1e30), mx[at])
                new = jnp.maximum(old, top)
                probs = jnp.exp2(scores - new)
                fade = jnp.exp2(old - new)
                mx[at] = new
                total = jnp.sum(probs, axis=0, keepdims=True)
                sm[at] = jnp.where(i < 2, total, sm[at] * fade + total)
                mixed = jnp.dot(vt[...], probs.astype(jnp.bfloat16), preferred_element_type=jnp.float32)

                @pl.when(i < 2)
                def _():
                    acc[at] = mixed

                @pl.when(i >= 2)
                def _():
                    acc[at] = acc[at] * fade + mixed

                return 0

            lax.fori_loop(0, group_size, one, 0)

        for at, jj in ((8, 0), (9, 1)):
            @pl.when(i == at)
            def _():
                finish(jj)

        return 0

    lax.fori_loop(0, 10, step, 0)

    per_side = CHUNKS // 2

    def first_copy(b, c, r):
        return copy(sum1.at[b, c, r], sum1.at[b, c, r], s1_send.at[b, c, r], s1_recv.at[b, c, r], s, near)

    def second_copy(b, c, r):
        return copy(sum2.at[b, c, r], sum2.at[b, c, r], s2_send.at[b, c, r], s2_recv.at[b, c, r], s, far)

    def third_copy(g, c, r):
        return copy(give3.at[g, c, r], got3.at[g, c, r], s3_send.at[g, c, r], s3_recv.at[g, c, r], mate, h)

    def odd(b):
        return lax.rem(b // groups + h, 2) == 1

    def product(source, b, c, n, r):
        side = r // per_side
        at = pl.multiple_of(lax.rem(r, per_side) * part, part)

        def weights(lo):
            return jnp.concatenate([wbuf[b, c + i, lo:lo + half, :] for i in range(n)], axis=1)

        y = (jnp.dot(source[side, 0, pl.ds(at, part), :], weights(0), preferred_element_type=jnp.float32)
             + jnp.dot(source[side, 1, pl.ds(at, part), :], weights(half), preferred_element_type=jnp.float32))
        return [y[:, i * wcp:(i + 1) * wcp] for i in range(n)]

    def compute(b, c, n, lo, hi):
        @pl.when(odd(b))
        def _():
            def chunk(r, _):
                for i, y in enumerate(product(both, b, c, n, r)):
                    sum1[b, c + i, r] = y.astype(jnp.bfloat16)
                    first_copy(b, c + i, r).start()
                return 0

            lax.fori_loop(lo, hi, chunk, 0, unroll=True)

        @pl.when(jnp.logical_not(odd(b)))
        def _():
            def chunk(r, _):
                for i, y in enumerate(product(both, b, c, n, r)):
                    tmp[c + i, r] = y
                return 0

            lax.fori_loop(lo, hi, chunk, 0, unroll=True)

    def settle(b, c, lo, hi):
        @pl.when(jnp.logical_not(odd(b)))
        def _():
            home = b // groups == h
            g = lax.rem(b, groups)

            def one(r, _):
                first_copy(b, c, r).wait_recv()
                y = tmp[c, r] + sum1[b, c, r].astype(jnp.float32)

                @pl.when(home)
                def _():
                    keep[g, c, r] = y

                @pl.when(jnp.logical_not(home))
                def _():
                    sum2[b, c, r] = y.astype(jnp.bfloat16)
                    second_copy(b, c, r).start()

                return 0

            lax.fori_loop(lo, hi, one, 0)

    def block_side(b, side):
        lo, hi = side * per_side, (side + 1) * per_side

        def first(k, _):
            compute(b, k * wide, wide, lo, hi)
            return 0

        def second(c, _):
            settle(b, c, lo, hi)
            return 0

        lax.fori_loop(0, pieces // wide, first, 0)
        lax.fori_loop(0, pieces, second, 0)

    def lent_first(c, r):
        return copy(lsum1.at[c, r], lsum1.at[c, r], l1_send.at[c, r], l1_recv.at[c, r], s, near)

    def lent_result(c, r):
        return copy(lsum2.at[c, r], lgot.at[c, r], l2_send.at[c, r], l2_recv.at[c, r], right, h)

    def lent_second(c, r):
        return copy(lgot.at[c, r], sum2.at[0, c, r], s2_send.at[0, c, r], s2_recv.at[0, c, r], s, far)

    def help_step(c, side):
        at = side * per_side

        @pl.when(odd(0))
        def _():
            def chunk(r, _):
                lsum1[c, r] = product(lent, 0, c, 1, r)[0].astype(jnp.bfloat16)
                lent_first(c, r).start()
                return 0

            lax.fori_loop(at, at + per_side, chunk, 0, unroll=True)

        @pl.when(jnp.logical_not(odd(0)))
        def _():
            def chunk(r, _):
                tmp[c, r] = product(lent, 0, c, 1, r)[0]
                return 0

            lax.fori_loop(at, at + per_side, chunk, 0, unroll=True)

            def settle(r, _):
                lent_first(c, r).wait_recv()
                lsum2[c, r] = (tmp[c, r] + lsum1[c, r].astype(jnp.float32)).astype(jnp.bfloat16)
                lent_result(c, r).start()
                return 0

            lax.fori_loop(at, at + per_side, settle, 0)

    def in_order(one):
        def early(side):
            def each(c, _):
                one(c, side)
                return 0

            lax.fori_loop(0, pieces - 1, each, 0)

        early(1)
        early(0)
        for side in range(2):
            one(pieces - 1, side)

    def take_lent(c, side):
        @pl.when(jnp.logical_not(odd(0)))
        def _():
            def each(r, _):
                lent_result(c, r).wait_recv()

                @pl.when(h == 0)
                def _():
                    keep[0, c, r] = lgot[c, r].astype(jnp.float32)

                @pl.when(h != 0)
                def _():
                    lent_second(c, r).start()

                return 0

            lax.fori_loop(side * per_side, (side + 1) * per_side, each, 0)

    def block_at(e):
        d = (e + 1) // 2
        from_up = lax.rem(e, 2) == 1
        b = jnp.where(from_up, p + d, p - d)
        return jnp.clip(b, 0, pairs - 1), (b >= 0) & (b < pairs), from_up, d

    def take_early(c):
        @pl.when(has_down)
        def _():
            take_right(0, c)

        @pl.when(p + 2 < pairs)
        def _():
            take_left(1, c)

    def own_side(e, _):
        for c in range(pieces):
            @pl.when(e == (c if c < min(pieces - 1, 2) else 2))
            def _():
                take_early(c)

        b, exists, _, _ = block_at(e)

        @pl.when(exists)
        def _():
            block_side(b, 1)

        return 0

    lax.fori_loop(0, 4, own_side, 0)

    for j in range(2):
        attn_copy(j).wait_recv()
        if j == 0:
            @pl.when(is_last)
            def _():
                lend_other(0, both.at[0, 0], left).start()

    def other_side(e, _):
        b, exists, _, _ = block_at(e)

        @pl.when(exists)
        def _():
            block_side(b, 0)

        @pl.when(is_helper & (e == 0))
        def _():
            for j in range(2):
                lend_own(j).wait_recv()
            lend_other(1, lent.at[1, 1], mate).start()

        return 0

    lax.fori_loop(0, 4, other_side, 0)

    def block_step(e, _):
        b, exists, from_up, d = block_at(e)
        helped = is_last & (b == 0)
        helping = is_helper & (b == 0)

        @pl.when(exists & jnp.logical_not(helped))
        def _():
            def one(c, _):
                @pl.when(from_up)
                def _():
                    take_left(d - 1, c)

                @pl.when(jnp.logical_not(from_up))
                def _():
                    take_right(d - 1, c)

                @pl.when(helping & (c == pieces - 1))
                def _():
                    for j in range(2):
                        lend_other(j, both.at[0, 0], left).wait_recv()

                    def other(k, _):
                        help_step(k, 0)
                        return 0

                    lax.fori_loop(0, pieces, other, 0)
                    help_step(c, 1)

                compute(b, c, 1, 0, CHUNKS)
                settle(b, c, 0, CHUNKS)

                @pl.when(helping & (c < pieces - 1))
                def _():
                    help_step(c, 1)

                return 0

            lax.fori_loop(0, pieces, one, 0)

        @pl.when(helped)
        def _():
            in_order(take_lent)

        return 0

    lax.fori_loop(4, 2 * pairs - 1, block_step, 0)

    def result(g, c, r):
        b = h * groups + g
        second_copy(b, c, r).wait_recv()
        return (keep[g, c, r] + sum2[b, c, r].astype(jnp.float32)).astype(jnp.bfloat16)

    def place(g, c, r, member, value):
        at = pl.multiple_of(lax.rem(r, per_side) * part, part)
        first_col = pl.multiple_of((2 * g + member) * wc + c * wcp, wcp)
        out_ref[pl.ds(at, part), pl.ds(first_col, wcp)] = value

    for g in range(groups):
        def pass_on(c, side):
            for r in range(side * per_side, (side + 1) * per_side):
                value = result(g, c, r)
                if side:
                    place(g, c, r, m, value)
                else:
                    give3[g, c, r] = value
                    third_copy(g, c, r).start()

        in_order(pass_on)

    for g in range(groups):
        def take_in(c, _):
            for r in range(per_side):
                third_copy(g, c, r).wait_recv()
                place(g, c, r, 1 - m, got3[g, c, r])
            return 0

        lax.fori_loop(0, pieces, take_in, 0)

    for j in range(2):
        @pl.when(has_next)
        def _():
            for c in kv_copies(0, 2, j, kvz_send.at[0], right):
                c.wait_send()

        @pl.when((s >= 2) & has_next)
        def _():
            for c in kv_copies(2, 4, j, kvz_send.at[1], right):
                c.wait_send()

        @pl.when(m == 0)
        def _():
            for c in kv_copies(0, 1, j, kvy_send.at[0], mate):
                c.wait_send()

        @pl.when(s >= 2)
        def _():
            for c in kv_copies(2, 3 - 2 * m, j, kvy_send.at[1], mate):
                c.wait_send()

        @pl.when((s >= 4) & (m == 1))
        def _():
            for c in kv_copies(4, 3, j, kvy_send.at[2], mate):
                c.wait_send()

        attn_copy(j).wait_send()

    def drain(b, _):
        def one(c, _):
            @pl.when(has_down & (p + b < pairs))
            def _():
                left_copy(b, c).wait_send()

            @pl.when(has_up & (p - b >= 0) & jnp.logical_not(is_helper & (p == b)))
            def _():
                right_copy(b, c).wait_send()

            for r in range(CHUNKS):
                @pl.when(odd(b) & jnp.logical_not(is_last & (b == 0)))
                def _():
                    first_copy(b, c, r).wait_send()

                @pl.when(jnp.logical_not(odd(b)) & (b // groups != h))
                def _():
                    second_copy(b, c, r).wait_send()

            return 0

        return lax.fori_loop(0, pieces, one, 0)

    lax.fori_loop(0, pairs, drain, 0)

    @pl.when(is_last)
    def _():
        for j in range(2):
            lend_own(j).wait_send()
        lend_other(0, both.at[0, 0], left).wait_send()

    @pl.when(is_helper)
    def _():
        lend_other(1, lent.at[1, 1], mate).wait_send()

        def one(c, _):
            for r in range(CHUNKS):
                @pl.when(odd(0))
                def _():
                    lent_first(c, r).wait_send()

                @pl.when(jnp.logical_not(odd(0)))
                def _():
                    lent_result(c, r).wait_send()

            return 0

        lax.fori_loop(0, pieces, one, 0)

    for g in range(groups):
        def sent(c, _):
            for r in range(per_side):
                third_copy(g, c, r).wait_send()
            return 0

        lax.fori_loop(0, pieces, sent, 0)


def body(n_seq, queries, keys, values, doc_lengths, out_weight):
    rows, width = queries.shape
    kv_width = keys.shape[1]
    depth, wc = out_weight.shape
    pairs = n_seq // 2
    groups = pairs // 4
    heads = width // DH
    part = rows * 2 // CHUNKS
    wcp = min(PIECE, wc)
    pieces = wc // wcp
    slots = -(-(MOST - 1) // rows) + 1
    vmem = pl.BlockSpec(memory_space=pltpu.VMEM)
    hbm = pl.BlockSpec(memory_space=pl.ANY)
    bf, f32, dma = jnp.bfloat16, jnp.float32, pltpu.SemaphoreType.DMA
    return pl.pallas_call(
        functools.partial(kernel, n_seq),
        out_shape=jax.ShapeDtypeStruct((rows, wc * 2 * (pairs // 4)), bf),
        in_specs=[pl.BlockSpec(memory_space=pltpu.SMEM), vmem, hbm, hbm, hbm],
        out_specs=vmem,
        scratch_shapes=[
            pltpu.VMEM((slots, rows, kv_width), bf),
            pltpu.VMEM((slots, rows, kv_width), bf),
            pltpu.VMEM((pairs, pieces, depth, wcp), bf),
            pltpu.VMEM((rows, rows), f32),
            pltpu.VMEM((DH, rows), bf),
            pltpu.VMEM((heads, 1, rows), f32),
            pltpu.VMEM((heads, 1, rows), f32),
            pltpu.VMEM((heads, DH, rows), f32),
            pltpu.VMEM((2, 2, rows, width // 2), bf),
            pltpu.VMEM((pieces, CHUNKS, part, wcp), f32),
            pltpu.VMEM((groups, pieces, CHUNKS, part, wcp), f32),
            pltpu.VMEM((pairs, pieces, CHUNKS, part, wcp), bf),
            pltpu.VMEM((pairs, pieces, CHUNKS, part, wcp), bf),
            pltpu.VMEM((groups, pieces, CHUNKS // 2, part, wcp), bf),
            pltpu.VMEM((groups, pieces, CHUNKS // 2, part, wcp), bf),
            pltpu.VMEM((2, 2, rows, width // 2), bf),
            pltpu.VMEM((pieces, CHUNKS, part, wcp), bf),
            pltpu.VMEM((pieces, CHUNKS, part, wcp), bf),
            pltpu.VMEM((pieces, CHUNKS, part, wcp), bf),
            dma((2 + pieces,)), dma((2, 2, 2)), dma((3, 2, 2)), dma((slots, 2, 2)),
            dma((pairs, pieces)), dma((pairs, pieces)), dma((pairs, pieces)), dma((pairs, pieces)),
            dma((2,)), dma((2,)),
            dma((pairs, pieces, CHUNKS)), dma((pairs, pieces, CHUNKS)),
            dma((pairs, pieces, CHUNKS)), dma((pairs, pieces, CHUNKS)),
            dma((groups, pieces, CHUNKS // 2)), dma((groups, pieces, CHUNKS // 2)),
            dma((2, 2)), dma((2, 2)), dma((pieces, CHUNKS)), dma((pieces, CHUNKS)),
            dma((pieces, CHUNKS)), dma((pieces, CHUNKS)),
        ],
        compiler_params=pltpu.CompilerParams(
            collective_id=0, has_side_effects=True, vmem_limit_bytes=56 * 1024 * 1024
        ),
    )(doc_lengths, queries, keys, values, out_weight)


def solution(mesh):
    return jax.shard_map(
        functools.partial(body, mesh.shape["seq"]),
        mesh=mesh,
        in_specs=(P("seq", "head"), P("seq", "head"), P("seq", "head"), P(), P("head", "seq")),
        out_specs=P("seq", "head"),
        check_vma=False,
    )
```

```python
import functools
import math

import jax
import jax.numpy as jnp
from jax import lax
from jax.experimental import pallas as pl
from jax.experimental.pallas import tpu as pltpu
from jax.sharding import PartitionSpec as P

HQ = 32
KV = 8
DH = 128
MOST = 2048
CHUNKS = 4
PIECE = 128
MESH = pl.DeviceIdType.MESH


def kernel(
    n_seq, lens_ref, q_hbm, k_hbm, v_hbm, w_hbm, out_hbm,
    q_ref, out_ref, kbuf, vbuf, wbuf, bias, vt, mx, sm, acc, both,
    tmp, keep, sum1, sum2, give3, got3, lent, lsum1, lsum2, lgot,
    load_sem, out_sem, kvz_send, kvy_send, kv_recv, wl_send, wl_recv, wr_send, wr_recv,
    at_send, at_recv, s1_send, s1_recv, s2_send, s2_recv, s3_send, s3_recv,
    la_send, la_recv, l1_send, l1_recv, l2_send, l2_recv,
):
    s, h = lax.axis_index("seq"), lax.axis_index("head")
    pairs = n_seq // 2
    p, m = s // 2, lax.rem(s, 2)
    mate = s + 1 - 2 * m
    right = lax.rem(p + 1, pairs) * 2 + m
    left = lax.rem(p + pairs - 1, pairs) * 2 + m
    near = h + 1 - 2 * lax.rem(h, 2)
    far = lax.rem(h + 2, 4)
    rows = q_ref.shape[0]
    depth, wc = w_hbm.shape
    pieces, wcp = wbuf.shape[1], wbuf.shape[3]
    half = depth // 2
    groups = pairs // 4
    group_size = HQ // KV
    part = rows * 2 // CHUNKS
    wide = 2 if pieces % 2 == 0 else 1
    has_up, has_down = p + 1 < pairs, p >= 1
    is_last, is_helper = p == pairs - 1, p == pairs - 2
    scale = DH ** (-0.5) * math.log2(math.e)

    def copy(src, dst, send, recv, seq, head):
        return pltpu.make_async_remote_copy(
            src_ref=src, dst_ref=dst, send_sem=send, recv_sem=recv,
            device_id={"seq": seq, "head": head}, device_id_type=MESH,
        )

    def kv_copies(src_slot, dst_slot, j, send, target):
        cols = pl.ds(pl.multiple_of(j * DH, DH), DH)
        return [
            copy(buf.at[src_slot, :, cols], buf.at[dst_slot, :, cols],
                 send.at[j, c], kv_recv.at[dst_slot, j, c], target, h)
            for c, buf in enumerate((kbuf, vbuf))
        ]

    def w_copy(block, c, step, send, recv, target):
        piece = wbuf.at[block, c]
        return copy(piece, piece, send.at[step], recv.at[step, c], target, h)

    def left_copy(step, c):
        return w_copy(jnp.minimum(p + step, pairs - 1), c, step, wl_send, wl_recv, left)

    def right_copy(step, c):
        return w_copy(jnp.maximum(p - step, 0), c, step, wr_send, wr_recv, right)

    loads = [
        pltpu.make_async_copy(k_hbm, kbuf.at[0], load_sem.at[0]),
        pltpu.make_async_copy(v_hbm, vbuf.at[0], load_sem.at[1]),
    ] + [
        pltpu.make_async_copy(w_hbm.at[:, c * wcp:(c + 1) * wcp], wbuf.at[p, c], load_sem.at[3 + c])
        for c in range(pieces)
    ] + [pltpu.make_async_copy(q_hbm, q_ref, load_sem.at[2])]
    for load in loads:
        load.start()

    barrier = pltpu.get_barrier_semaphore()
    for seq, head in ((mate, h), (left, h), (right, h), (s, near), (s, far)):
        pl.semaphore_signal(barrier, inc=1, device_id={"seq": seq, "head": head}, device_id_type=MESH)
    pl.semaphore_wait(barrier, 5)

    loads[0].wait()
    loads[1].wait()
    has_next = s + 2 < n_seq
    for j in range(2):
        @pl.when(has_next)
        def _():
            for c in kv_copies(0, 2, j, kvz_send.at[0], right):
                c.start()

        @pl.when(m == 0)
        def _():
            for c in kv_copies(0, 1, j, kvy_send.at[0], mate):
                c.start()

    for load in loads[2:-1]:
        load.wait()

    @pl.when(has_down)
    def _():
        for c in range(pieces):
            left_copy(0, c).start()

    q_pos = s * rows + lax.broadcasted_iota(jnp.int32, (1, rows), 1)
    start = jnp.int32(0)
    first = jnp.zeros((1, rows), jnp.int32)
    for d in range(1, lens_ref.shape[0]):
        start = start + lens_ref[d - 1]
        first = jnp.where(q_pos >= start, start, first)

    loads[-1].wait()

    def attn_copy(j):
        return copy(both.at[1, j], both.at[0, j], at_send.at[j], at_recv.at[j], mate, h)

    def lend_own(j):
        return copy(both.at[1, j], lent.at[1, j], la_send.at[0, j], la_recv.at[0, j], left, h)

    def lend_other(j, source, target):
        return copy(source, lent.at[0, j], la_send.at[1, j], la_recv.at[1, j], target, h)

    def finish(j):
        def one(g, _):
            i = j * group_size + g
            full = jnp.transpose(acc[i] / sm[i])
            both[1, j, :, pl.ds(pl.multiple_of(g * DH, DH), DH)] = full.astype(jnp.bfloat16)
            return 0

        lax.fori_loop(0, group_size, one, 0)
        @pl.when(is_last)
        def _():
            lend_own(j).start()

    def take_left(t, c):
        left_copy(t, c).wait_recv()

        @pl.when(has_down)
        def _():
            left_copy(t + 1, c).start()

    def take_right(t, c):
        right_copy(t, c).wait_recv()

        @pl.when(has_up & jnp.logical_not(is_helper & (p == t + 1)))
        def _():
            right_copy(t + 1, c).start()

    def step(i, _):
        k = jnp.maximum(i - 2, 0)
        w = lax.rem(k, 4)
        slot = jnp.where(i < 2, 0, 2 + 2 * (k // 4) - lax.rem(w, 2))
        j = jnp.where(i < 2, i, w // 2)

        @pl.when((i >= 2) & (s >= slot))
        def _():
            for c in kv_copies(slot, slot, j, kvz_send.at[0], right):
                c.wait_recv()

            @pl.when((slot == 2) & has_next)
            def _():
                for c in kv_copies(2, 4, j, kvz_send.at[1], right):
                    c.start()

            @pl.when(slot == 2)
            def _():
                for c in kv_copies(2, 3 - 2 * m, j, kvy_send.at[1], mate):
                    c.start()

            @pl.when((slot == 4) & (m == 1))
            def _():
                for c in kv_copies(4, 3, j, kvy_send.at[2], mate):
                    c.start()

        @pl.when(i == 8)
        def _():
            attn_copy(0).start()

        @pl.when((i == 4) & has_up)
        def _():
            for c in range(pieces):
                right_copy(0, c).start()

        for c in range(pieces):
            @pl.when((i == 11 - 2 * (pieces - c)) & has_up)
            def _():
                take_left(0, c)

        @pl.when(s >= slot)
        def _():
            cols = pl.ds(pl.multiple_of(j * DH, DH), DH)
            k_pos = (s - slot) * rows + lax.broadcasted_iota(jnp.int32, (rows, rows), 0)
            bias[...] = jnp.where((k_pos >= first) & (k_pos <= q_pos), 0.0, -1e30)
            vt[...] = jnp.transpose(vbuf[slot, :, cols])

            def one(g, _):
                at = j * group_size + g
                q = q_ref[:, pl.ds(pl.multiple_of(at * DH, DH), DH)]
                scores = lax.dot_general(
                    kbuf[slot, :, cols], q, (((1,), (1,)), ((), ())),
                    preferred_element_type=jnp.float32,
                ) * scale + bias[...]
                top = jnp.max(scores, axis=0, keepdims=True)
                old = jnp.where(i < 2, jnp.full_like(top, -1e30), mx[at])
                new = jnp.maximum(old, top)
                probs = jnp.exp2(scores - new)
                fade = jnp.exp2(old - new)
                mx[at] = new
                total = jnp.sum(probs, axis=0, keepdims=True)
                sm[at] = jnp.where(i < 2, total, sm[at] * fade + total)
                mixed = jnp.dot(vt[...], probs.astype(jnp.bfloat16), preferred_element_type=jnp.float32)

                @pl.when(i < 2)
                def _():
                    acc[at] = mixed

                @pl.when(i >= 2)
                def _():
                    acc[at] = acc[at] * fade + mixed

                return 0

            lax.fori_loop(0, group_size, one, 0)

        for at, jj in ((7, 0), (9, 1)):
            @pl.when(i == at)
            def _():
                finish(jj)

        return 0

    lax.fori_loop(0, 10, step, 0)
    attn_copy(1).start()

    per_side = CHUNKS // 2

    def first_copy(b, c, r):
        return copy(sum1.at[b, c, r], sum1.at[b, c, r], s1_send.at[b], s1_recv.at[b, c, r], s, near)

    def second_copy(b, c, r):
        return copy(sum2.at[b, c, r], sum2.at[b, c, r], s2_send.at[b], s2_recv.at[b, c, r], s, far)

    def third_copy(g, c, r):
        return copy(give3.at[g, c, r], got3.at[g, c, r], s3_send.at[g], s3_recv.at[g, c, r], mate, h)

    def odd(b):
        return lax.rem(b // groups + h, 2) == 1

    def product(source, b, c, n, r):
        side = r // per_side
        at = pl.multiple_of(lax.rem(r, per_side) * part, part)

        def weights(lo):
            return jnp.concatenate([wbuf[b, c + i, lo:lo + half, :] for i in range(n)], axis=1)

        y = (jnp.dot(source[side, 0, pl.ds(at, part), :], weights(0), preferred_element_type=jnp.float32)
             + jnp.dot(source[side, 1, pl.ds(at, part), :], weights(half), preferred_element_type=jnp.float32))
        return [y[:, i * wcp:(i + 1) * wcp] for i in range(n)]

    def compute(b, slot, c, n, lo, hi):
        @pl.when(odd(b))
        def _():
            def chunk(r, _):
                for i, y in enumerate(product(both, b, c, n, r)):
                    sum1[b, c + i, r] = y.astype(jnp.bfloat16)
                return 0

            lax.fori_loop(lo, hi, chunk, 0, unroll=True)
            for r in range(lo, hi):
                for i in range(n):
                    first_copy(b, c + i, r).start()

        @pl.when(jnp.logical_not(odd(b)))
        def _():
            def chunk(r, _):
                for i, y in enumerate(product(both, b, c, n, r)):
                    tmp[slot, c + i, r] = y
                return 0

            lax.fori_loop(lo, hi, chunk, 0, unroll=True)

    def settle(b, slot, c, lo, hi):
        @pl.when(jnp.logical_not(odd(b)))
        def _():
            home = b // groups == h
            g = lax.rem(b, groups)

            def one(r, _):
                first_copy(b, c, r).wait_recv()
                y = tmp[slot, c, r] + sum1[b, c, r].astype(jnp.float32)

                @pl.when(home)
                def _():
                    keep[g, c, r] = y

                @pl.when(jnp.logical_not(home))
                def _():
                    sum2[b, c, r] = y.astype(jnp.bfloat16)
                    second_copy(b, c, r).start()

                return 0

            lax.fori_loop(lo, hi, one, 0)

    def early_compute(e, side):
        b, exists, _, _ = block_at(e)

        @pl.when(exists)
        def _():
            def one(k, _):
                compute(b, e, k * wide, wide, side * per_side, (side + 1) * per_side)
                return 0

            lax.fori_loop(0, pieces // wide, one, 0)

    def early_settle(e, side):
        b, exists, _, _ = block_at(e)

        @pl.when(exists)
        def _():
            def one(c, _):
                settle(b, e, c, side * per_side, (side + 1) * per_side)
                return 0

            lax.fori_loop(0, pieces, one, 0)

    def lent_first(c, r):
        return copy(lsum1.at[c, r], lsum1.at[c, r], l1_send.at[0], l1_recv.at[c, r], s, near)

    def lent_result(c, r):
        return copy(lsum2.at[c, r], lgot.at[c, r], l2_send.at[0], l2_recv.at[c, r], right, h)

    def lent_second(c, r):
        return copy(lgot.at[c, r], sum2.at[0, c, r], s2_send.at[0], s2_recv.at[0, c, r], s, far)

    def help_step(c, side):
        at = side * per_side

        @pl.when(odd(0))
        def _():
            def chunk(r, _):
                lsum1[c, r] = product(lent, 0, c, 1, r)[0].astype(jnp.bfloat16)
                return 0

            lax.fori_loop(at, at + per_side, chunk, 0, unroll=True)
            for r in range(at, at + per_side):
                lent_first(c, r).start()

        @pl.when(jnp.logical_not(odd(0)))
        def _():
            def chunk(r, _):
                tmp[4, c, r] = product(lent, 0, c, 1, r)[0]
                return 0

            lax.fori_loop(at, at + per_side, chunk, 0, unroll=True)

            def add(r, _):
                lent_first(c, r).wait_recv()
                lsum2[c, r] = (tmp[4, c, r] + lsum1[c, r].astype(jnp.float32)).astype(jnp.bfloat16)
                lent_result(c, r).start()
                return 0

            lax.fori_loop(at, at + per_side, add, 0)

    def in_order(one):
        def early(side):
            def each(c, _):
                one(c, side)
                return 0

            lax.fori_loop(0, pieces - 1, each, 0)

        early(1)
        early(0)
        for side in range(2):
            one(pieces - 1, side)

    def take_lent(c, side):
        @pl.when(jnp.logical_not(odd(0)) & (h != 0))
        def _():
            def each(r, _):
                lent_result(c, r).wait_recv()
                lent_second(c, r).start()
                return 0

            lax.fori_loop(side * per_side, (side + 1) * per_side, each, 0)

    def block_at(e):
        d = (e + 1) // 2
        from_up = lax.rem(e, 2) == 1
        b = jnp.where(from_up, p + d, p - d)
        return jnp.clip(b, 0, pairs - 1), (b >= 0) & (b < pairs), from_up, d

    def take_early(c):
        @pl.when(has_down)
        def _():
            take_right(0, c)

        @pl.when(p + 2 < pairs)
        def _():
            take_left(1, c)

    def own_side(e, _):
        for c in range(pieces):
            @pl.when(e == (c if c < min(pieces - 1, 2) else 2))
            def _():
                take_early(c)

        early_compute(e, 1)

        @pl.when(e > 0)
        def _():
            early_settle(e - 1, 1)

        return 0

    lax.fori_loop(0, 4, own_side, 0)
    early_settle(3, 1)

    for j in range(2):
        attn_copy(j).wait_recv()
        if j == 0:
            @pl.when(is_last)
            def _():
                lend_other(0, both.at[0, 0], left).start()

    def other_side(e, _):
        early_compute(e, 0)

        @pl.when(is_helper & (e == 0))
        def _():
            for j in range(2):
                lend_own(j).wait_recv()
            lend_other(1, lent.at[1, 1], mate).start()

        @pl.when(e > 0)
        def _():
            early_settle(e - 1, 0)

        return 0

    lax.fori_loop(0, 4, other_side, 0)
    early_settle(3, 0)

    def block_step(e, _):
        b, exists, from_up, d = block_at(e)
        helped = is_last & (b == 0)
        helping = is_helper & (b == 0)

        @pl.when(exists & jnp.logical_not(helped))
        def _():
            def one(c, _):
                @pl.when(from_up)
                def _():
                    take_left(d - 1, c)

                @pl.when(jnp.logical_not(from_up))
                def _():
                    take_right(d - 1, c)

                @pl.when(helping & (c < pieces - 1))
                def _():
                    help_step(c, 1)

                @pl.when(helping & (c == pieces - 1))
                def _():
                    for j in range(2):
                        lend_other(j, both.at[0, 0], left).wait_recv()

                    def other(k, _):
                        help_step(k, 0)
                        return 0

                    lax.fori_loop(0, pieces, other, 0)
                    help_step(c, 1)

                compute(b, 4, c, 1, 0, CHUNKS)
                settle(b, 4, c, 0, CHUNKS)
                return 0

            lax.fori_loop(0, pieces, one, 0)

        @pl.when(helped)
        def _():
            in_order(take_lent)

        return 0

    lax.fori_loop(4, 2 * pairs - 1, block_step, 0)

    def result(g, c, r, store):
        def usual():
            second_copy(h * groups + g, c, r).wait_recv()
            store((keep[g, c, r] + sum2[h * groups + g, c, r].astype(jnp.float32)).astype(jnp.bfloat16))

        if g > 0:
            usual()
            return
        helped = is_last & (h == 0)
        pl.when(jnp.logical_not(helped))(usual)

        @pl.when(helped)
        def _():
            lent_result(c, r).wait_recv()
            second_copy(0, c, r).wait_recv()
            store((lgot[c, r].astype(jnp.float32) + sum2[0, c, r].astype(jnp.float32)).astype(jnp.bfloat16))

    def columns(g, c, member):
        return pl.ds(pl.multiple_of((2 * g + member) * wc + c * wcp, wcp), wcp)

    def place(g, c, r, member, value):
        at = pl.multiple_of(lax.rem(r, per_side) * part, part)
        out_ref[pl.ds(at, part), columns(g, c, member)] = value

    def out_copy(g, c, member):
        cols = columns(g, c, member)
        return pltpu.make_async_copy(out_ref.at[:, cols], out_hbm.at[:, cols], out_sem.at[0])

    for g in range(groups):
        def pass_on(c, side):
            for r in range(side * per_side, (side + 1) * per_side):
                def store(value):
                    if side:
                        place(g, c, r, m, value)
                    else:
                        give3[g, c, r] = value
                        third_copy(g, c, r).start()

                result(g, c, r, store)
            if side:
                out_copy(g, c, m).start()

        in_order(pass_on)

    for g in range(groups):
        def take_in(c, _):
            for r in range(per_side):
                third_copy(g, c, r).wait_recv()
                place(g, c, r, 1 - m, got3[g, c, r])
            out_copy(g, c, 1 - m).start()
            return 0

        lax.fori_loop(0, pieces, take_in, 0)

    for j in range(2):
        @pl.when(has_next)
        def _():
            for c in kv_copies(0, 2, j, kvz_send.at[0], right):
                c.wait_send()

        @pl.when((s >= 2) & has_next)
        def _():
            for c in kv_copies(2, 4, j, kvz_send.at[1], right):
                c.wait_send()

        @pl.when(m == 0)
        def _():
            for c in kv_copies(0, 1, j, kvy_send.at[0], mate):
                c.wait_send()

        @pl.when(s >= 2)
        def _():
            for c in kv_copies(2, 3 - 2 * m, j, kvy_send.at[1], mate):
                c.wait_send()

        @pl.when((s >= 4) & (m == 1))
        def _():
            for c in kv_copies(4, 3, j, kvy_send.at[2], mate):
                c.wait_send()

        attn_copy(j).wait_send()

    def sent(ref, sem):
        copy(ref, ref, sem, s1_recv.at[0, 0, 0], s, near).wait_send()

    def drain(b, _):
        @pl.when(has_down & (p + b < pairs))
        def _():
            sent(wbuf.at[b], wl_send.at[b])

        @pl.when(has_up & (p - b >= 0) & jnp.logical_not(is_helper & (p == b)))
        def _():
            sent(wbuf.at[b], wr_send.at[b])

        lent_block = is_last & (b == 0)

        @pl.when(odd(b) & jnp.logical_not(lent_block))
        def _():
            sent(sum1.at[b], s1_send.at[b])

        @pl.when(jnp.logical_not(odd(b)) & (b // groups != h) & jnp.logical_not(lent_block))
        def _():
            sent(sum2.at[b], s2_send.at[b])

        return 0

    lax.fori_loop(0, pairs, drain, 0)
    for g in range(groups):
        sent(give3.at[g], s3_send.at[g])

    pltpu.make_async_copy(out_ref, out_hbm, out_sem.at[0]).wait()

    @pl.when(is_last)
    def _():
        for j in range(2):
            lend_own(j).wait_send()
        lend_other(0, both.at[0, 0], left).wait_send()

        @pl.when(jnp.logical_not(odd(0)) & (h != 0))
        def _():
            sent(lgot, s2_send.at[0])

    @pl.when(is_helper)
    def _():
        lend_other(1, lent.at[1, 1], mate).wait_send()

        @pl.when(odd(0))
        def _():
            sent(lsum1, l1_send.at[0])

        @pl.when(jnp.logical_not(odd(0)))
        def _():
            sent(lsum2, l2_send.at[0])


def body(n_seq, queries, keys, values, doc_lengths, out_weight):
    rows, width = queries.shape
    kv_width = keys.shape[1]
    depth, wc = out_weight.shape
    pairs = n_seq // 2
    groups = pairs // 4
    heads = width // DH
    part = rows * 2 // CHUNKS
    wcp = min(PIECE, wc)
    pieces = wc // wcp
    slots = -(-(MOST - 1) // rows) + 1
    hbm = pl.BlockSpec(memory_space=pl.ANY)
    bf, f32, dma = jnp.bfloat16, jnp.float32, pltpu.SemaphoreType.DMA
    return pl.pallas_call(
        functools.partial(kernel, n_seq),
        out_shape=jax.ShapeDtypeStruct((rows, wc * 2 * (pairs // 4)), bf),
        in_specs=[pl.BlockSpec(memory_space=pltpu.SMEM), hbm, hbm, hbm, hbm],
        out_specs=hbm,
        scratch_shapes=[
            pltpu.VMEM((rows, width), bf),
            pltpu.VMEM((rows, wc * 2 * groups), bf),
            pltpu.VMEM((slots, rows, kv_width), bf),
            pltpu.VMEM((slots, rows, kv_width), bf),
            pltpu.VMEM((pairs, pieces, depth, wcp), bf),
            pltpu.VMEM((rows, rows), f32),
            pltpu.VMEM((DH, rows), bf),
            pltpu.VMEM((heads, 1, rows), f32),
            pltpu.VMEM((heads, 1, rows), f32),
            pltpu.VMEM((heads, DH, rows), f32),
            pltpu.VMEM((2, 2, rows, width // 2), bf),
            pltpu.VMEM((5, pieces, CHUNKS, part, wcp), f32),
            pltpu.VMEM((groups, pieces, CHUNKS, part, wcp), f32),
            pltpu.VMEM((pairs, pieces, CHUNKS, part, wcp), bf),
            pltpu.VMEM((pairs, pieces, CHUNKS, part, wcp), bf),
            pltpu.VMEM((groups, pieces, CHUNKS // 2, part, wcp), bf),
            pltpu.VMEM((groups, pieces, CHUNKS // 2, part, wcp), bf),
            pltpu.VMEM((2, 2, rows, width // 2), bf),
            pltpu.VMEM((pieces, CHUNKS, part, wcp), bf),
            pltpu.VMEM((pieces, CHUNKS, part, wcp), bf),
            pltpu.VMEM((pieces, CHUNKS, part, wcp), bf),
            dma((3 + pieces,)), dma((1,)), dma((2, 2, 2)), dma((3, 2, 2)), dma((slots, 2, 2)),
            dma((pairs,)), dma((pairs, pieces)), dma((pairs,)), dma((pairs, pieces)),
            dma((2,)), dma((2,)), dma((pairs,)), dma((pairs, pieces, CHUNKS)),
            dma((pairs,)), dma((pairs, pieces, CHUNKS)),
            dma((groups,)), dma((groups, pieces, CHUNKS // 2)),
            dma((2, 2)), dma((2, 2)), dma((1,)), dma((pieces, CHUNKS)),
            dma((1,)), dma((pieces, CHUNKS)),
        ],
        compiler_params=pltpu.CompilerParams(
            collective_id=0, has_side_effects=True, vmem_limit_bytes=56 * 1024 * 1024
        ),
    )(doc_lengths, queries, keys, values, out_weight)


def solution(mesh):
    return jax.shard_map(
        functools.partial(body, mesh.shape["seq"]),
        mesh=mesh,
        in_specs=(P("seq", "head"), P("seq", "head"), P("seq", "head"), P(), P("head", "seq")),
        out_specs=P("seq", "head"),
        check_vma=False,
    )
```

```python
import functools
import math

import jax
import jax.numpy as jnp
from jax import lax
from jax.experimental import pallas as pl
from jax.experimental.pallas import tpu as pltpu
from jax.sharding import PartitionSpec as P

HQ = 32
KV = 8
DH = 128
MOST = 2048
CHUNKS = 4
PIECE = 128
MESH = pl.DeviceIdType.MESH


def kernel(
    n_seq, lens_ref, q_hbm, k_hbm, v_hbm, w_hbm, out_hbm,
    q_ref, out_ref, kvbuf, wbuf, bias, vt, mx, sm, acc, both,
    tmp, keep, sum1, sum2, give3, got3, lent, lsum1, lsum2, lgot,
    load_sem, out_sem, kvz_send, kvy_send, kv_recv, wl_send, wl_recv, wr_send, wr_recv,
    at_send, at_recv, s1_send, s1_recv, s2_send, s2_recv, s3_send, s3_recv,
    la_send, la_recv, l1_send, l1_recv, l2_send, l2_recv,
):
    s, h = lax.axis_index("seq"), lax.axis_index("head")
    pairs = n_seq // 2
    p, m = s // 2, lax.rem(s, 2)
    mate = s + 1 - 2 * m
    right = lax.rem(p + 1, pairs) * 2 + m
    left = lax.rem(p + pairs - 1, pairs) * 2 + m
    near = h + 1 - 2 * lax.rem(h, 2)
    far = lax.rem(h + 2, 4)
    rows = q_ref.shape[0]
    depth, wc = w_hbm.shape
    pieces, wcp = wbuf.shape[1], wbuf.shape[3]
    half = depth // 2
    groups = pairs // 4
    group_size = HQ // KV
    part = rows * 2 // CHUNKS
    wide = 2 if pieces % 2 == 0 else 1
    split = pieces // 2 if pieces % (2 * wide) == 0 else pieces
    has_up, has_down = p + 1 < pairs, p >= 1
    is_last, is_helper = p == pairs - 1, p == pairs - 2
    scale = DH ** (-0.5) * math.log2(math.e)

    def copy(src, dst, send, recv, seq, head):
        return pltpu.make_async_remote_copy(
            src_ref=src, dst_ref=dst, send_sem=send, recv_sem=recv,
            device_id={"seq": seq, "head": head}, device_id_type=MESH,
        )

    def kv_copy(src_slot, dst_slot, j, send, target):
        cols = pl.ds(pl.multiple_of(j * DH, DH), DH)
        return copy(kvbuf.at[src_slot, :, :, cols], kvbuf.at[dst_slot, :, :, cols],
                    send.at[j], kv_recv.at[dst_slot, j], target, h)

    def w_copy(block, c, step, send, recv, target):
        piece = wbuf.at[block, c]
        return copy(piece, piece, send.at[step], recv.at[step, c], target, h)

    def left_copy(step, c):
        return w_copy(jnp.minimum(p + step, pairs - 1), c, step, wl_send, wl_recv, left)

    def right_copy(step, c):
        return w_copy(jnp.maximum(p - step, 0), c, step, wr_send, wr_recv, right)

    loads = [
        pltpu.make_async_copy(k_hbm, kvbuf.at[0, 0], load_sem.at[0]),
        pltpu.make_async_copy(v_hbm, kvbuf.at[0, 1], load_sem.at[1]),
    ] + [
        pltpu.make_async_copy(w_hbm.at[:, c * wcp:(c + 1) * wcp], wbuf.at[p, c], load_sem.at[3])
        for c in range(pieces)
    ] + [pltpu.make_async_copy(q_hbm, q_ref, load_sem.at[2])]
    for load in loads:
        load.start()

    barrier = pltpu.get_barrier_semaphore()
    for seq, head in ((mate, h), (left, h), (right, h), (s, near), (s, far)):
        pl.semaphore_signal(barrier, inc=1, device_id={"seq": seq, "head": head}, device_id_type=MESH)
    pl.semaphore_wait(barrier, 5)

    loads[0].wait()
    loads[1].wait()
    has_next = s + 2 < n_seq
    for j in range(2):
        @pl.when(has_next)
        def _():
            kv_copy(0, 2, j, kvz_send.at[0], right).start()

        @pl.when(m == 0)
        def _():
            kv_copy(0, 1, j, kvy_send.at[0], mate).start()

    pltpu.make_async_copy(wbuf.at[p], wbuf.at[p], load_sem.at[3]).wait()

    @pl.when(has_down)
    def _():
        for c in range(pieces):
            left_copy(0, c).start()

    q_pos = s * rows + lax.broadcasted_iota(jnp.int32, (1, rows), 1)
    start = jnp.int32(0)
    first = jnp.zeros((1, rows), jnp.int32)
    for d in range(1, lens_ref.shape[0]):
        start = start + lens_ref[d - 1]
        first = jnp.where(q_pos >= start, start, first)

    loads[-1].wait()

    def attn_copy(j):
        return copy(both.at[1, j], both.at[0, j], at_send.at[j], at_recv.at[j], mate, h)

    def lend_own(j):
        return copy(both.at[1, j], lent.at[1, j], la_send.at[0, j], la_recv.at[0, j], left, h)

    def lend_other(j, source, target):
        return copy(source, lent.at[0, j], la_send.at[1, j], la_recv.at[1, j], target, h)

    def finish(j):
        def one(g, _):
            i = j * group_size + g
            full = jnp.transpose(acc[i] / sm[i])
            both[1, j, :, pl.ds(pl.multiple_of(g * DH, DH), DH)] = full.astype(jnp.bfloat16)
            return 0

        lax.fori_loop(0, group_size, one, 0)
        @pl.when(is_last)
        def _():
            lend_own(j).start()

    def take_left(t, c):
        left_copy(t, c).wait_recv()

        @pl.when(has_down)
        def _():
            left_copy(t + 1, c).start()

    def take_right(t, c):
        right_copy(t, c).wait_recv()

        @pl.when(has_up & jnp.logical_not(is_helper & (p == t + 1)))
        def _():
            right_copy(t + 1, c).start()

    def step(i, _):
        k = jnp.maximum(i - 2, 0)
        w = lax.rem(k, 4)
        slot = jnp.where(i < 2, 0, 2 + 2 * (k // 4) - lax.rem(w, 2))
        j = jnp.where(i < 2, i, w // 2)

        @pl.when((i >= 2) & (s >= slot))
        def _():
            kv_copy(slot, slot, j, kvz_send.at[0], right).wait_recv()

            @pl.when((slot == 2) & has_next)
            def _():
                kv_copy(2, 4, j, kvz_send.at[1], right).start()

            @pl.when(slot == 2)
            def _():
                kv_copy(2, 3 - 2 * m, j, kvy_send.at[1], mate).start()

            @pl.when((slot == 4) & (m == 1))
            def _():
                kv_copy(4, 3, j, kvy_send.at[2], mate).start()

        @pl.when(i == 8)
        def _():
            attn_copy(0).start()

        @pl.when((i == 4) & has_up)
        def _():
            for c in range(split):
                right_copy(0, c).start()

            @pl.when(jnp.logical_not(is_helper))
            def _():
                for c in range(split, pieces):
                    right_copy(0, c).start()

        for c in range(pieces):
            @pl.when((i == 11 - 2 * (pieces - c)) & has_up)
            def _():
                take_left(0, c)

        @pl.when(s >= slot)
        def _():
            cols = pl.ds(pl.multiple_of(j * DH, DH), DH)
            k_pos = (s - slot) * rows + lax.broadcasted_iota(jnp.int32, (rows, rows), 0)
            bias[...] = jnp.where((k_pos >= first) & (k_pos <= q_pos), 0.0, -1e30)
            vt[...] = jnp.transpose(kvbuf[slot, 1, :, cols])

            def one(g, _):
                at = j * group_size + g
                q = q_ref[:, pl.ds(pl.multiple_of(at * DH, DH), DH)]
                scores = lax.dot_general(
                    kvbuf[slot, 0, :, cols], q, (((1,), (1,)), ((), ())),
                    preferred_element_type=jnp.float32,
                ) * scale + bias[...]
                top = jnp.max(scores, axis=0, keepdims=True)
                old = jnp.where(i < 2, jnp.full_like(top, -1e30), mx[at])
                new = jnp.maximum(old, top)
                probs = jnp.exp2(scores - new)
                fade = jnp.exp2(old - new)
                mx[at] = new
                total = jnp.sum(probs, axis=0, keepdims=True)
                sm[at] = jnp.where(i < 2, total, sm[at] * fade + total)
                mixed = jnp.dot(vt[...], probs.astype(jnp.bfloat16), preferred_element_type=jnp.float32)

                @pl.when(i < 2)
                def _():
                    acc[at] = mixed

                @pl.when(i >= 2)
                def _():
                    acc[at] = acc[at] * fade + mixed

                return 0

            lax.fori_loop(0, group_size, one, 0)

        for at, jj in ((7, 0), (9, 1)):
            @pl.when(i == at)
            def _():
                finish(jj)

        return 0

    lax.fori_loop(0, 10, step, 0)
    attn_copy(1).start()

    per_side = CHUNKS // 2

    def rows_of(side):
        return pl.ds(side * per_side, per_side)

    def first_copy(b, c, side):
        piece = sum1.at[b, c, rows_of(side)]
        return copy(piece, piece, s1_send.at[b], s1_recv.at[b, c, side], s, near)

    def second_copy(b, c, side):
        piece = sum2.at[b, c, rows_of(side)]
        return copy(piece, piece, s2_send.at[b], s2_recv.at[b, c, side], s, far)

    def third_copy(g, c):
        return copy(give3.at[g, c], got3.at[g, c], s3_send.at[g], s3_recv.at[g, c], mate, h)

    def odd(b):
        return lax.rem(b // groups + h, 2) == 1

    def product(source, b, c, n, r):
        side = r // per_side
        at = pl.multiple_of(lax.rem(r, per_side) * part, part)

        def weights(lo):
            return jnp.concatenate([wbuf[b, c + i, lo:lo + half, :] for i in range(n)], axis=1)

        y = (jnp.dot(source[side, 0, pl.ds(at, part), :], weights(0), preferred_element_type=jnp.float32)
             + jnp.dot(source[side, 1, pl.ds(at, part), :], weights(half), preferred_element_type=jnp.float32))
        return [y[:, i * wcp:(i + 1) * wcp] for i in range(n)]

    def compute(b, slot, c, n, sides):
        lo, hi = sides[0] * per_side, (sides[-1] + 1) * per_side

        @pl.when(odd(b))
        def _():
            def chunk(r, _):
                for i, y in enumerate(product(both, b, c, n, r)):
                    sum1[b, c + i, r] = y.astype(jnp.bfloat16)
                return 0

            lax.fori_loop(lo, hi, chunk, 0, unroll=True)
            for side in sides:
                for i in range(n):
                    first_copy(b, c + i, side).start()

        @pl.when(jnp.logical_not(odd(b)))
        def _():
            def chunk(r, _):
                for i, y in enumerate(product(both, b, c, n, r)):
                    tmp[slot, c + i, r] = y
                return 0

            lax.fori_loop(lo, hi, chunk, 0, unroll=True)

    def settle(b, slot, c, sides):
        @pl.when(jnp.logical_not(odd(b)))
        def _():
            home = b // groups == h
            g = lax.rem(b, groups)

            def one(side, _):
                first_copy(b, c, side).wait_recv()

                @pl.when(home)
                def _():
                    for k in range(per_side):
                        r = side * per_side + k
                        keep[g, c, r] = tmp[slot, c, r] + sum1[b, c, r].astype(jnp.float32)

                @pl.when(jnp.logical_not(home))
                def _():
                    for k in range(per_side):
                        r = side * per_side + k
                        sum2[b, c, r] = (tmp[slot, c, r] + sum1[b, c, r].astype(jnp.float32)).astype(jnp.bfloat16)
                    second_copy(b, c, side).start()

                return 0

            lax.fori_loop(sides[0], sides[-1] + 1, one, 0)

    def early_pieces(e):
        return jnp.where(is_last & (e == 2), split, pieces)

    def early_compute(e, side):
        b, exists, _, _ = block_at(e)

        @pl.when(exists)
        def _():
            def one(k, _):
                compute(b, e, k * wide, wide, (side,))
                return 0

            lax.fori_loop(0, early_pieces(e) // wide, one, 0)

    def early_settle(e, side):
        b, exists, _, _ = block_at(e)

        @pl.when(exists)
        def _():
            def one(c, _):
                settle(b, e, c, (side,))
                return 0

            lax.fori_loop(0, early_pieces(e), one, 0)

    def lent_first(c, side):
        piece = lsum1.at[c, rows_of(side)]
        return copy(piece, piece, l1_send.at[0], l1_recv.at[c, side], s, near)

    def lent_result(c, r):
        return copy(lsum2.at[c, r], lgot.at[c, r], l2_send.at[0], l2_recv.at[c, r], right, h)

    def lent_second(c, r):
        return copy(lgot.at[c, r], sum2.at[0, c, r], s2_send.at[0], s2_recv.at[0, c, r // per_side], s, far)

    def help_step(c, side):
        at = side * per_side

        @pl.when(odd(0))
        def _():
            def chunk(r, _):
                lsum1[c, r] = product(lent, 0, c, 1, r)[0].astype(jnp.bfloat16)
                return 0

            lax.fori_loop(at, at + per_side, chunk, 0, unroll=True)
            lent_first(c, side).start()

        @pl.when(jnp.logical_not(odd(0)))
        def _():
            def chunk(r, _):
                tmp[4, c, r] = product(lent, 0, c, 1, r)[0]
                return 0

            lax.fori_loop(at, at + per_side, chunk, 0, unroll=True)

            lent_first(c, side).wait_recv()

            def add(r, _):
                lsum2[c, r] = (tmp[4, c, r] + lsum1[c, r].astype(jnp.float32)).astype(jnp.bfloat16)
                lent_result(c, r).start()
                return 0

            lax.fori_loop(at, at + per_side, add, 0)

    def in_order(one):
        def early(side):
            def each(c, _):
                one(c, side)
                return 0

            lax.fori_loop(0, pieces - 1, each, 0)

        early(1)
        early(0)
        for side in range(2):
            one(pieces - 1, side)

    def take_lent(c, side):
        def each(r, _):
            lent_result(c, r).wait_recv()
            lent_second(c, r).start()
            return 0

        lax.fori_loop(side * per_side, (side + 1) * per_side, each, 0)

    def block_at(e):
        d = (e + 1) // 2
        from_up = lax.rem(e, 2) == 1
        b = jnp.where(from_up, p + d, p - d)
        return jnp.clip(b, 0, pairs - 1), (b >= 0) & (b < pairs), from_up, d

    def take_early(c):
        @pl.when(has_down & (jnp.logical_not(is_last) | (c < split)))
        def _():
            take_right(0, c)

        if c == pieces - 1:
            @pl.when(is_helper)
            def _():
                for k in range(split, pieces):
                    right_copy(0, k).start()

        @pl.when(p + 2 < pairs)
        def _():
            take_left(1, c)

    def own_side(e, _):
        for c in range(pieces):
            @pl.when(e == (c if c < min(pieces - 1, 2) else 2))
            def _():
                take_early(c)

        early_compute(e, 1)

        @pl.when(e > 0)
        def _():
            early_settle(e - 1, 1)

        return 0

    lax.fori_loop(0, 4, own_side, 0)
    early_settle(3, 1)

    for j in range(2):
        attn_copy(j).wait_recv()
        if j == 0:
            @pl.when(is_last)
            def _():
                lend_other(0, both.at[0, 0], left).start()

    late = is_last | is_helper

    def other_side(k, _):
        order = (2, 1, 0, 3)

        def at(k):
            return sum(jnp.where(k == i, e, 0) for i, e in enumerate(order))

        @pl.when(jnp.logical_not(late) | (is_helper & (k == 0)))
        def _():
            early_compute(at(k), 0)

        @pl.when(is_helper & (k == 0))
        def _():
            for j in range(2):
                lend_own(j).wait_recv()
            lend_other(1, lent.at[1, 1], mate).start()

        @pl.when((jnp.logical_not(late) & (k > 0)) | (is_helper & (k == 1)))
        def _():
            early_settle(at(k - 1), 0)

        return 0

    lax.fori_loop(0, 4, other_side, 0)

    @pl.when(jnp.logical_not(late))
    def _():
        early_settle(3, 0)

    def block_step(e, _):
        b, exists, from_up, d = block_at(e)
        helped = is_last & (b == 0)
        helping = is_helper & (b == 0)
        last_block = 2 * (pairs - 2)

        @pl.when(exists & jnp.logical_not(helped))
        def _():
            def one(c, _):
                @pl.when(from_up)
                def _():
                    take_left(d - 1, c)

                @pl.when(jnp.logical_not(from_up))
                def _():
                    take_right(d - 1, c)

                @pl.when(helping & (c < pieces - 1))
                def _():
                    help_step(c, 1)

                @pl.when(helping & (c == pieces - 1))
                def _():
                    for j in range(2):
                        lend_other(j, both.at[0, 0], left).wait_recv()

                    def other(k, _):
                        help_step(k, 0)
                        return 0

                    lax.fori_loop(0, pieces, other, 0)
                    help_step(c, 1)

                compute(b, 4, c, 1, (0, 1))
                settle(b, 4, c, (0, 1))

                @pl.when(late & (e == last_block) & (c == min(1, pieces - 1)))
                def _():
                    early_compute(0, 0)

                    @pl.when(is_helper)
                    def _():
                        early_compute(1, 0)

                    @pl.when(is_last)
                    def _():
                        early_compute(2, 0)

                    early_settle(0, 0)

                    @pl.when(is_helper)
                    def _():
                        early_settle(1, 0)

                    @pl.when(is_last)
                    def _():
                        early_settle(2, 0)

                return 0

            lax.fori_loop(0, pieces, one, 0)

        @pl.when(is_last & (e == 4))
        def _():
            def rest(c, _):
                take_right(0, c)
                compute(p - 1, 4, c, 1, (0, 1))
                settle(p - 1, 4, c, (0, 1))
                return 0

            lax.fori_loop(split, pieces, rest, 0)

        return 0

    lax.fori_loop(4, 2 * pairs - 1, block_step, 0)

    def result(g, c, side, store):
        b = h * groups + g
        at = [side * per_side + k for k in range(per_side)]

        def usual():
            second_copy(b, c, side).wait_recv()
            for r in at:
                store(r, (keep[g, c, r] + sum2[b, c, r].astype(jnp.float32)).astype(jnp.bfloat16))

        if g > 0:
            usual()
            return
        helped = is_last & (h == 0)
        pl.when(jnp.logical_not(helped))(usual)

        @pl.when(helped)
        def _():
            for r in at:
                lent_result(c, r).wait_recv()
            second_copy(0, c, side).wait_recv()
            for r in at:
                store(r, (lgot[c, r].astype(jnp.float32) + sum2[0, c, r].astype(jnp.float32)).astype(jnp.bfloat16))

    def columns(g, c, member):
        return pl.ds(pl.multiple_of((2 * g + member) * wc + c * wcp, wcp), wcp)

    def place(g, c, r, member, value):
        at = pl.multiple_of(lax.rem(r, per_side) * part, part)
        out_ref[pl.ds(at, part), columns(g, c, member)] = value

    def out_copy(g, c, member):
        cols = columns(g, c, member)
        return pltpu.make_async_copy(out_ref.at[:, cols], out_hbm.at[:, cols], out_sem.at[0])

    def pass_on(c, side):
        for g in range(groups):
            def store(r, value):
                if side:
                    place(g, c, r, m, value)
                else:
                    give3[g, c, r] = value

            result(g, c, side, store)
            if side:
                out_copy(g, c, m).start()
            else:
                third_copy(g, c).start()

    lender = is_last & jnp.logical_not(odd(0)) & (h != 0)

    @pl.when(lender)
    def _():
        def each(one, sides):
            def body(c, _):
                for side in sides:
                    one(c, side)
                return 0

            lax.fori_loop(0, pieces - 1, body, 0)

        each(take_lent, (1,))
        each(pass_on, (0, 1))
        each(take_lent, (0,))
        for one in (pass_on, take_lent):
            for side in range(2):
                one(pieces - 1, side)

    @pl.when(jnp.logical_not(lender))
    def _():
        in_order(pass_on)

    for g in range(groups):
        def take_in(c, _):
            third_copy(g, c).wait_recv()
            for r in range(per_side):
                place(g, c, r, 1 - m, got3[g, c, r])
            out_copy(g, c, 1 - m).start()
            return 0

        lax.fori_loop(0, pieces, take_in, 0)

    for j in range(2):
        @pl.when(has_next)
        def _():
            kv_copy(0, 2, j, kvz_send.at[0], right).wait_send()

        @pl.when((s >= 2) & has_next)
        def _():
            kv_copy(2, 4, j, kvz_send.at[1], right).wait_send()

        @pl.when(m == 0)
        def _():
            kv_copy(0, 1, j, kvy_send.at[0], mate).wait_send()

        @pl.when(s >= 2)
        def _():
            kv_copy(2, 3 - 2 * m, j, kvy_send.at[1], mate).wait_send()

        @pl.when((s >= 4) & (m == 1))
        def _():
            kv_copy(4, 3, j, kvy_send.at[2], mate).wait_send()

        attn_copy(j).wait_send()

    def sent(ref, sem):
        copy(ref, ref, sem, s1_recv.at[0, 0, 0], s, near).wait_send()

    def drain(b, _):
        @pl.when(has_down & (p + b < pairs))
        def _():
            sent(wbuf.at[b], wl_send.at[b])

        @pl.when(has_up & (p - b >= 0) & jnp.logical_not(is_helper & (p == b)))
        def _():
            sent(wbuf.at[b], wr_send.at[b])

        lent_block = is_last & (b == 0)

        @pl.when(odd(b) & jnp.logical_not(lent_block))
        def _():
            sent(sum1.at[b], s1_send.at[b])

        @pl.when(jnp.logical_not(odd(b)) & (b // groups != h) & jnp.logical_not(lent_block))
        def _():
            sent(sum2.at[b], s2_send.at[b])

        return 0

    lax.fori_loop(0, pairs, drain, 0)
    for g in range(groups):
        sent(give3.at[g], s3_send.at[g])

    pltpu.make_async_copy(out_ref, out_hbm, out_sem.at[0]).wait()

    @pl.when(is_last)
    def _():
        for j in range(2):
            lend_own(j).wait_send()
        lend_other(0, both.at[0, 0], left).wait_send()

        @pl.when(jnp.logical_not(odd(0)) & (h != 0))
        def _():
            sent(lgot, s2_send.at[0])

    @pl.when(is_helper)
    def _():
        lend_other(1, lent.at[1, 1], mate).wait_send()

        @pl.when(odd(0))
        def _():
            sent(lsum1, l1_send.at[0])

        @pl.when(jnp.logical_not(odd(0)))
        def _():
            sent(lsum2, l2_send.at[0])


def body(n_seq, queries, keys, values, doc_lengths, out_weight):
    rows, width = queries.shape
    kv_width = keys.shape[1]
    depth, wc = out_weight.shape
    pairs = n_seq // 2
    groups = pairs // 4
    heads = width // DH
    part = rows * 2 // CHUNKS
    wcp = min(PIECE, wc)
    pieces = wc // wcp
    slots = -(-(MOST - 1) // rows) + 1
    hbm = pl.BlockSpec(memory_space=pl.ANY)
    bf, f32, dma = jnp.bfloat16, jnp.float32, pltpu.SemaphoreType.DMA
    return pl.pallas_call(
        functools.partial(kernel, n_seq),
        out_shape=jax.ShapeDtypeStruct((rows, wc * 2 * (pairs // 4)), bf),
        in_specs=[pl.BlockSpec(memory_space=pltpu.SMEM), hbm, hbm, hbm, hbm],
        out_specs=hbm,
        scratch_shapes=[
            pltpu.VMEM((rows, width), bf),
            pltpu.VMEM((rows, wc * 2 * groups), bf),
            pltpu.VMEM((slots, 2, rows, kv_width), bf),
            pltpu.VMEM((pairs, pieces, depth, wcp), bf),
            pltpu.VMEM((rows, rows), f32),
            pltpu.VMEM((DH, rows), bf),
            pltpu.VMEM((heads, 1, rows), f32),
            pltpu.VMEM((heads, 1, rows), f32),
            pltpu.VMEM((heads, DH, rows), f32),
            pltpu.VMEM((2, 2, rows, width // 2), bf),
            pltpu.VMEM((5, pieces, CHUNKS, part, wcp), f32),
            pltpu.VMEM((groups, pieces, CHUNKS, part, wcp), f32),
            pltpu.VMEM((pairs, pieces, CHUNKS, part, wcp), bf),
            pltpu.VMEM((pairs, pieces, CHUNKS, part, wcp), bf),
            pltpu.VMEM((groups, pieces, CHUNKS // 2, part, wcp), bf),
            pltpu.VMEM((groups, pieces, CHUNKS // 2, part, wcp), bf),
            pltpu.VMEM((2, 2, rows, width // 2), bf),
            pltpu.VMEM((pieces, CHUNKS, part, wcp), bf),
            pltpu.VMEM((pieces, CHUNKS, part, wcp), bf),
            pltpu.VMEM((pieces, CHUNKS, part, wcp), bf),
            dma((4,)), dma((1,)), dma((2, 2)), dma((3, 2)), dma((slots, 2)),
            dma((pairs - 1,)), dma((pairs - 1, pieces)), dma((pairs - 1,)), dma((pairs - 1, pieces)),
            dma((2,)), dma((2,)), dma((pairs,)), dma((pairs, pieces, 2)), dma((pairs,)), dma((pairs, pieces, 2)),
            dma((groups,)), dma((groups, pieces)),
            dma((2, 2)), dma((2, 2)), dma((1,)), dma((pieces, 2)), dma((1,)), dma((pieces, CHUNKS)),
        ],
        compiler_params=pltpu.CompilerParams(
            collective_id=0, has_side_effects=True, vmem_limit_bytes=56 * 1024 * 1024
        ),
    )(doc_lengths, queries, keys, values, out_weight)


def solution(mesh):
    return jax.shard_map(
        functools.partial(body, mesh.shape["seq"]),
        mesh=mesh,
        in_specs=(P("seq", "head"), P("seq", "head"), P("seq", "head"), P(), P("head", "seq")),
        out_specs=P("seq", "head"),
        check_vma=False,
    )
```

```python
import functools
import math

import jax
import jax.numpy as jnp
from jax import lax
from jax.experimental import pallas as pl
from jax.experimental.pallas import tpu as pltpu
from jax.sharding import PartitionSpec as P

HQ = 32
KV = 8
DH = 128
MOST = 2048
CHUNKS = 4
PIECE = 128
MESH = pl.DeviceIdType.MESH


def kernel(
    n_seq, lens_ref, q_hbm, k_hbm, v_hbm, w_hbm, out_hbm,
    q_ref, out_ref, kvbuf, wbuf, bias, vt, mx, sm, acc, both,
    tmp, keep, sum1, sum2, give3, got3, lent, lsum1, lsum2, lgot,
    load_sem, out_sem, kvz_send, kvy_send, kv_recv, wl_send, wl_recv, wr_send, wr_recv,
    at_send, at_recv, s1_send, s1_recv, s2_send, s2_recv, s3_send, s3_recv,
    la_send, la_recv, l1_send, l1_recv, l2_send, l2_recv,
):
    s, h = lax.axis_index("seq"), lax.axis_index("head")
    pairs = n_seq // 2
    p, m = s // 2, lax.rem(s, 2)
    mate = s + 1 - 2 * m
    right = lax.rem(p + 1, pairs) * 2 + m
    left = lax.rem(p + pairs - 1, pairs) * 2 + m
    near = h + 1 - 2 * lax.rem(h, 2)
    far = lax.rem(h + 2, 4)
    rows = q_ref.shape[0]
    depth, wc = w_hbm.shape
    pieces, wcp = wbuf.shape[1], wbuf.shape[3]
    half = depth // 2
    groups = pairs // 4
    group_size = HQ // KV
    part = rows * 2 // CHUNKS
    wide = 2 if pieces % 2 == 0 else 1
    split = pieces // 2 if pieces % (2 * wide) == 0 else pieces
    has_up, has_down = p + 1 < pairs, p >= 1
    is_last, is_helper = p == pairs - 1, p == pairs - 2
    scale = DH ** (-0.5) * math.log2(math.e)

    def copy(src, dst, send, recv, seq, head):
        return pltpu.make_async_remote_copy(
            src_ref=src, dst_ref=dst, send_sem=send, recv_sem=recv,
            device_id={"seq": seq, "head": head}, device_id_type=MESH,
        )

    def kv_copy(src_slot, dst_slot, j, send, target):
        cols = pl.ds(pl.multiple_of(j * DH, DH), DH)
        return copy(kvbuf.at[src_slot, :, :, cols], kvbuf.at[dst_slot, :, :, cols],
                    send.at[j], kv_recv.at[dst_slot, j], target, h)

    def w_copy(block, c, step, send, recv, target):
        piece = wbuf.at[block, c]
        return copy(piece, piece, send.at[step], recv.at[step, c], target, h)

    def left_copy(step, c):
        return w_copy(jnp.minimum(p + step, pairs - 1), c, step, wl_send, wl_recv, left)

    def right_copy(step, c):
        return w_copy(jnp.maximum(p - step, 0), c, step, wr_send, wr_recv, right)

    loads = [
        pltpu.make_async_copy(k_hbm, kvbuf.at[0, 0], load_sem.at[0]),
        pltpu.make_async_copy(v_hbm, kvbuf.at[0, 1], load_sem.at[1]),
    ] + [
        pltpu.make_async_copy(w_hbm.at[:, c * wcp:(c + 1) * wcp], wbuf.at[p, c], load_sem.at[3])
        for c in range(pieces)
    ] + [pltpu.make_async_copy(q_hbm, q_ref, load_sem.at[2])]
    for load in loads:
        load.start()

    barrier = pltpu.get_barrier_semaphore()
    for seq, head in ((mate, h), (left, h), (right, h), (s, near), (s, far)):
        pl.semaphore_signal(barrier, inc=1, device_id={"seq": seq, "head": head}, device_id_type=MESH)
    pl.semaphore_wait(barrier, 5)

    loads[0].wait()
    loads[1].wait()
    has_next = s + 2 < n_seq
    for j in range(2):
        @pl.when(has_next)
        def _():
            kv_copy(0, 2, j, kvz_send.at[0], right).start()

        @pl.when(m == 0)
        def _():
            kv_copy(0, 1, j, kvy_send.at[0], mate).start()

    pltpu.make_async_copy(wbuf.at[p], wbuf.at[p], load_sem.at[3]).wait()

    @pl.when(has_down)
    def _():
        for c in range(pieces):
            left_copy(0, c).start()

    q_pos = s * rows + lax.broadcasted_iota(jnp.int32, (1, rows), 1)
    start = jnp.int32(0)
    first = jnp.zeros((1, rows), jnp.int32)
    for d in range(1, lens_ref.shape[0]):
        start = start + lens_ref[d - 1]
        first = jnp.where(q_pos >= start, start, first)

    loads[-1].wait()

    def attn_copy(j):
        return copy(both.at[1, j], both.at[0, j], at_send.at[j], at_recv.at[j], mate, h)

    def lend_own(j):
        return copy(both.at[1, j], lent.at[1, j], la_send.at[0, j], la_recv.at[0, j], left, h)

    def lend_other(j, source, target):
        return copy(source, lent.at[0, j], la_send.at[1, j], la_recv.at[1, j], target, h)

    def finish(j):
        def one(g, _):
            i = j * group_size + g
            full = jnp.transpose(acc[i] / sm[i])
            both[1, j, :, pl.ds(pl.multiple_of(g * DH, DH), DH)] = full.astype(jnp.bfloat16)
            return 0

        lax.fori_loop(0, group_size, one, 0)
        @pl.when(is_last)
        def _():
            lend_own(j).start()

    def take_left(t, c):
        left_copy(t, c).wait_recv()

        @pl.when(has_down)
        def _():
            left_copy(t + 1, c).start()

    def take_right(t, c):
        right_copy(t, c).wait_recv()

        @pl.when(has_up & jnp.logical_not(is_helper & (p == t + 1)))
        def _():
            right_copy(t + 1, c).start()

    def step(i, _):
        k = jnp.maximum(i - 2, 0)
        w = lax.rem(k, 4)
        slot = jnp.where(i < 2, 0, 2 + 2 * (k // 4) - lax.rem(w, 2))
        j = jnp.where(i < 2, i, w // 2)

        @pl.when((i >= 2) & (s >= slot))
        def _():
            kv_copy(slot, slot, j, kvz_send.at[0], right).wait_recv()

            @pl.when((slot == 2) & has_next)
            def _():
                kv_copy(2, 4, j, kvz_send.at[1], right).start()

            @pl.when(slot == 2)
            def _():
                kv_copy(2, 3 - 2 * m, j, kvy_send.at[1], mate).start()

            @pl.when((slot == 4) & (m == 1))
            def _():
                kv_copy(4, 3, j, kvy_send.at[2], mate).start()

        @pl.when(i == 8)
        def _():
            attn_copy(0).start()

        @pl.when((i == 4) & has_up)
        def _():
            for c in range(split):
                right_copy(0, c).start()

            @pl.when(jnp.logical_not(is_helper))
            def _():
                for c in range(split, pieces):
                    right_copy(0, c).start()

        for c in range(pieces):
            @pl.when((i == 11 - 2 * (pieces - c)) & has_up)
            def _():
                take_left(0, c)

        @pl.when(s >= slot)
        def _():
            cols = pl.ds(pl.multiple_of(j * DH, DH), DH)
            k_pos = (s - slot) * rows + lax.broadcasted_iota(jnp.int32, (rows, rows), 0)
            bias[...] = jnp.where((k_pos >= first) & (k_pos <= q_pos), 0.0, -1e30)
            vt[...] = jnp.transpose(kvbuf[slot, 1, :, cols])

            def one(g, _):
                at = j * group_size + g
                q = q_ref[:, pl.ds(pl.multiple_of(at * DH, DH), DH)]
                scores = lax.dot_general(
                    kvbuf[slot, 0, :, cols], q, (((1,), (1,)), ((), ())),
                    preferred_element_type=jnp.float32,
                ) * scale + bias[...]
                top = jnp.max(scores, axis=0, keepdims=True)
                old = jnp.where(i < 2, jnp.full_like(top, -1e30), mx[at])
                new = jnp.maximum(old, top)
                probs = jnp.exp2(scores - new)
                fade = jnp.exp2(old - new)
                mx[at] = new
                total = jnp.sum(probs, axis=0, keepdims=True)
                sm[at] = jnp.where(i < 2, total, sm[at] * fade + total)
                mixed = jnp.dot(vt[...], probs.astype(jnp.bfloat16), preferred_element_type=jnp.float32)

                @pl.when(i < 2)
                def _():
                    acc[at] = mixed

                @pl.when(i >= 2)
                def _():
                    acc[at] = acc[at] * fade + mixed

                return 0

            lax.fori_loop(0, group_size, one, 0)

        for at, jj in ((7, 0), (9, 1)):
            @pl.when(i == at)
            def _():
                finish(jj)

        return 0

    lax.fori_loop(0, 10, step, 0)
    attn_copy(1).start()

    per_side = CHUNKS // 2

    def rows_of(side):
        return pl.ds(side * per_side, per_side)

    def first_copy(b, c, side):
        piece = sum1.at[b, c, rows_of(side)]
        return copy(piece, piece, s1_send.at[b], s1_recv.at[b, c, side], s, near)

    def second_copy(b, c, side):
        piece = sum2.at[b, c, rows_of(side)]
        return copy(piece, piece, s2_send.at[b], s2_recv.at[b, c, side], s, far)

    def third_copy(g, c):
        return copy(give3.at[g, c], got3.at[g, c], s3_send.at[g], s3_recv.at[g, c], mate, h)

    def odd(b):
        return lax.rem(b // groups + h, 2) == 1

    def product(source, b, c, n, r):
        side = r // per_side
        at = pl.multiple_of(lax.rem(r, per_side) * part, part)

        def weights(lo):
            return jnp.concatenate([wbuf[b, c + i, lo:lo + half, :] for i in range(n)], axis=1)

        y = (jnp.dot(source[side, 0, pl.ds(at, part), :], weights(0), preferred_element_type=jnp.float32)
             + jnp.dot(source[side, 1, pl.ds(at, part), :], weights(half), preferred_element_type=jnp.float32))
        return [y[:, i * wcp:(i + 1) * wcp] for i in range(n)]

    def compute(b, slot, c, n, sides):
        lo, hi = sides[0] * per_side, (sides[-1] + 1) * per_side

        @pl.when(odd(b))
        def _():
            def chunk(r, _):
                for i, y in enumerate(product(both, b, c, n, r)):
                    sum1[b, c + i, r] = y.astype(jnp.bfloat16)
                return 0

            lax.fori_loop(lo, hi, chunk, 0, unroll=True)
            for side in sides:
                for i in range(n):
                    first_copy(b, c + i, side).start()

        @pl.when(jnp.logical_not(odd(b)))
        def _():
            def chunk(r, _):
                for i, y in enumerate(product(both, b, c, n, r)):
                    tmp[slot, c + i, r] = y
                return 0

            lax.fori_loop(lo, hi, chunk, 0, unroll=True)

    def settle(b, slot, c, sides):
        @pl.when(jnp.logical_not(odd(b)))
        def _():
            home = b // groups == h
            g = lax.rem(b, groups)

            def one(side, _):
                first_copy(b, c, side).wait_recv()

                @pl.when(home)
                def _():
                    for k in range(per_side):
                        r = side * per_side + k
                        keep[g, c, r] = tmp[slot, c, r] + sum1[b, c, r].astype(jnp.float32)

                @pl.when(jnp.logical_not(home))
                def _():
                    for k in range(per_side):
                        r = side * per_side + k
                        sum2[b, c, r] = (tmp[slot, c, r] + sum1[b, c, r].astype(jnp.float32)).astype(jnp.bfloat16)
                    second_copy(b, c, side).start()

                return 0

            lax.fori_loop(sides[0], sides[-1] + 1, one, 0)

    def early_pieces(e):
        return jnp.where(is_last & (e == 2), split, pieces)

    def early_compute(e, side):
        b, exists, _, _ = block_at(e)

        @pl.when(exists)
        def _():
            def one(k, _):
                compute(b, e, k * wide, wide, (side,))
                return 0

            lax.fori_loop(0, early_pieces(e) // wide, one, 0)

    def early_settle(e, side):
        b, exists, _, _ = block_at(e)

        @pl.when(exists)
        def _():
            def one(c, _):
                settle(b, e, c, (side,))
                return 0

            lax.fori_loop(0, early_pieces(e), one, 0)

    def lent_first(c, side):
        piece = lsum1.at[c, rows_of(side)]
        return copy(piece, piece, l1_send.at[0], l1_recv.at[c, side], s, near)

    def lent_result(c, r):
        return copy(lsum2.at[c, r], lgot.at[c, r], l2_send.at[0], l2_recv.at[c, r], right, h)

    def lent_second(c, r):
        return copy(lgot.at[c, r], sum2.at[0, c, r], s2_send.at[0], s2_recv.at[0, c, r // per_side], s, far)

    def help_step(c, side):
        at = side * per_side

        @pl.when(odd(0))
        def _():
            def chunk(r, _):
                lsum1[c, r] = product(lent, 0, c, 1, r)[0].astype(jnp.bfloat16)
                return 0

            lax.fori_loop(at, at + per_side, chunk, 0, unroll=True)
            lent_first(c, side).start()

        @pl.when(jnp.logical_not(odd(0)))
        def _():
            def chunk(r, _):
                tmp[4, c, r] = product(lent, 0, c, 1, r)[0]
                return 0

            lax.fori_loop(at, at + per_side, chunk, 0, unroll=True)

            lent_first(c, side).wait_recv()

            def add(r, _):
                lsum2[c, r] = (tmp[4, c, r] + lsum1[c, r].astype(jnp.float32)).astype(jnp.bfloat16)
                lent_result(c, r).start()
                return 0

            lax.fori_loop(at, at + per_side, add, 0)

    lead = 1 if pieces > 1 else 0

    def over(one, side, lo, hi):
        def body(c, _):
            one(c, side)
            return 0

        lax.fori_loop(lo, hi, body, 0)

    def in_order(one):
        over(one, 1, 0, lead)
        over(one, 0, 0, pieces)
        over(one, 1, lead, pieces)

    def take_lent(c, side):
        def each(r, _):
            lent_result(c, r).wait_recv()
            lent_second(c, r).start()
            return 0

        lax.fori_loop(side * per_side, (side + 1) * per_side, each, 0)

    def block_at(e):
        d = (e + 1) // 2
        from_up = lax.rem(e, 2) == 1
        b = jnp.where(from_up, p + d, p - d)
        return jnp.clip(b, 0, pairs - 1), (b >= 0) & (b < pairs), from_up, d

    def take_early(c):
        @pl.when(has_down & (jnp.logical_not(is_last) | (c < split)))
        def _():
            take_right(0, c)

        if c == pieces - 1:
            @pl.when(is_helper)
            def _():
                for k in range(split, pieces):
                    right_copy(0, k).start()

        @pl.when(p + 2 < pairs)
        def _():
            take_left(1, c)

    def own_side(e, _):
        for c in range(pieces):
            @pl.when(e == (c if c < min(pieces - 1, 2) else 2))
            def _():
                take_early(c)

        early_compute(e, 1)

        @pl.when(e > 0)
        def _():
            early_settle(e - 1, 1)

        return 0

    lax.fori_loop(0, 4, own_side, 0)
    early_settle(3, 1)

    for j in range(2):
        attn_copy(j).wait_recv()
        if j == 0:
            @pl.when(is_last)
            def _():
                lend_other(0, both.at[0, 0], left).start()

    late = is_last | is_helper

    def other_side(k, _):
        order = (2, 1, 0, 3)

        def at(k):
            return sum(jnp.where(k == i, e, 0) for i, e in enumerate(order))

        @pl.when(jnp.logical_not(late) | (is_helper & (k == 0)))
        def _():
            early_compute(at(k), 0)

        @pl.when(is_helper & (k == 0))
        def _():
            for j in range(2):
                lend_own(j).wait_recv()
            lend_other(1, lent.at[1, 1], mate).start()

        @pl.when((jnp.logical_not(late) & (k > 0)) | (is_helper & (k == 1)))
        def _():
            early_settle(at(k - 1), 0)

        return 0

    lax.fori_loop(0, 4, other_side, 0)

    @pl.when(jnp.logical_not(late))
    def _():
        early_settle(3, 0)

    def block_step(e, _):
        b, exists, from_up, d = block_at(e)
        helped = is_last & (b == 0)
        helping = is_helper & (b == 0)
        last_block = 2 * (pairs - 2)

        @pl.when(exists & jnp.logical_not(helped))
        def _():
            def one(c, _):
                @pl.when(from_up)
                def _():
                    take_left(d - 1, c)

                @pl.when(jnp.logical_not(from_up))
                def _():
                    take_right(d - 1, c)

                @pl.when(helping & (c < lead))
                def _():
                    help_step(c, 1)

                @pl.when(helping & (c == pieces - 1))
                def _():
                    for j in range(2):
                        lend_other(j, both.at[0, 0], left).wait_recv()
                    over(help_step, 0, 0, pieces)

                compute(b, 4, c, 1, (0, 1))
                settle(b, 4, c, (0, 1))

                @pl.when(helping & (c == pieces - 1))
                def _():
                    over(help_step, 1, lead, pieces)

                @pl.when(late & (e == last_block) & (c == min(1, pieces - 1)))
                def _():
                    early_compute(0, 0)

                    @pl.when(is_helper)
                    def _():
                        early_compute(1, 0)

                    @pl.when(is_last)
                    def _():
                        early_compute(2, 0)

                    early_settle(0, 0)

                    @pl.when(is_helper)
                    def _():
                        early_settle(1, 0)

                    @pl.when(is_last)
                    def _():
                        early_settle(2, 0)

                return 0

            lax.fori_loop(0, pieces, one, 0)

        @pl.when(is_last & (e == 4))
        def _():
            def rest(c, _):
                take_right(0, c)
                compute(p - 1, 4, c, 1, (0, 1))
                settle(p - 1, 4, c, (0, 1))
                return 0

            lax.fori_loop(split, pieces, rest, 0)

        return 0

    lax.fori_loop(4, 2 * pairs - 1, block_step, 0)

    def result(g, c, side, store):
        b = h * groups + g
        at = [side * per_side + k for k in range(per_side)]

        def usual():
            second_copy(b, c, side).wait_recv()
            for r in at:
                store(r, (keep[g, c, r] + sum2[b, c, r].astype(jnp.float32)).astype(jnp.bfloat16))

        if g > 0:
            usual()
            return
        helped = is_last & (h == 0)
        pl.when(jnp.logical_not(helped))(usual)

        @pl.when(helped)
        def _():
            for r in at:
                lent_result(c, r).wait_recv()
            second_copy(0, c, side).wait_recv()
            for r in at:
                store(r, (lgot[c, r].astype(jnp.float32) + sum2[0, c, r].astype(jnp.float32)).astype(jnp.bfloat16))

    def columns(g, c, member):
        return pl.ds(pl.multiple_of((2 * g + member) * wc + c * wcp, wcp), wcp)

    def place(g, c, r, member, value):
        at = pl.multiple_of(lax.rem(r, per_side) * part, part)
        out_ref[pl.ds(at, part), columns(g, c, member)] = value

    def out_copy(g, c, member):
        cols = columns(g, c, member)
        return pltpu.make_async_copy(out_ref.at[:, cols], out_hbm.at[:, cols], out_sem.at[0])

    def pass_on(c, side):
        for g in range(groups):
            def store(r, value):
                if side:
                    place(g, c, r, m, value)
                else:
                    give3[g, c, r] = value

            result(g, c, side, store)
            if side:
                out_copy(g, c, m).start()
            else:
                third_copy(g, c).start()

    lender = is_last & jnp.logical_not(odd(0)) & (h != 0)

    @pl.when(lender)
    def _():
        over(take_lent, 1, 0, lead)
        for side in range(2):
            over(pass_on, side, 0, pieces - 1)
        over(take_lent, 0, 0, pieces)
        for side in range(2):
            pass_on(pieces - 1, side)
        over(take_lent, 1, lead, pieces)

    lent_to = is_last & (h == 0)

    @pl.when(lent_to)
    def _():
        in_order(pass_on)

    @pl.when(jnp.logical_not(lender | lent_to))
    def _():
        def each(c, _):
            pass_on(c, 0)
            pass_on(c, 1)
            return 0

        lax.fori_loop(0, pieces, each, 0)

    for g in range(groups):
        def take_in(c, _):
            third_copy(g, c).wait_recv()
            for r in range(per_side):
                place(g, c, r, 1 - m, got3[g, c, r])
            out_copy(g, c, 1 - m).start()
            return 0

        lax.fori_loop(0, pieces, take_in, 0)

    for j in range(2):
        @pl.when(has_next)
        def _():
            kv_copy(0, 2, j, kvz_send.at[0], right).wait_send()

        @pl.when((s >= 2) & has_next)
        def _():
            kv_copy(2, 4, j, kvz_send.at[1], right).wait_send()

        @pl.when(m == 0)
        def _():
            kv_copy(0, 1, j, kvy_send.at[0], mate).wait_send()

        @pl.when(s >= 2)
        def _():
            kv_copy(2, 3 - 2 * m, j, kvy_send.at[1], mate).wait_send()

        @pl.when((s >= 4) & (m == 1))
        def _():
            kv_copy(4, 3, j, kvy_send.at[2], mate).wait_send()

        attn_copy(j).wait_send()

    def sent(ref, sem):
        copy(ref, ref, sem, s1_recv.at[0, 0, 0], s, near).wait_send()

    def drain(b, _):
        @pl.when(has_down & (p + b < pairs))
        def _():
            sent(wbuf.at[b], wl_send.at[b])

        @pl.when(has_up & (p - b >= 0) & jnp.logical_not(is_helper & (p == b)))
        def _():
            sent(wbuf.at[b], wr_send.at[b])

        lent_block = is_last & (b == 0)

        @pl.when(odd(b) & jnp.logical_not(lent_block))
        def _():
            sent(sum1.at[b], s1_send.at[b])

        @pl.when(jnp.logical_not(odd(b)) & (b // groups != h) & jnp.logical_not(lent_block))
        def _():
            sent(sum2.at[b], s2_send.at[b])

        return 0

    lax.fori_loop(0, pairs, drain, 0)
    for g in range(groups):
        sent(give3.at[g], s3_send.at[g])

    pltpu.make_async_copy(out_ref, out_hbm, out_sem.at[0]).wait()

    @pl.when(is_last)
    def _():
        for j in range(2):
            lend_own(j).wait_send()
        lend_other(0, both.at[0, 0], left).wait_send()

        @pl.when(jnp.logical_not(odd(0)) & (h != 0))
        def _():
            sent(lgot, s2_send.at[0])

    @pl.when(is_helper)
    def _():
        lend_other(1, lent.at[1, 1], mate).wait_send()

        @pl.when(odd(0))
        def _():
            sent(lsum1, l1_send.at[0])

        @pl.when(jnp.logical_not(odd(0)))
        def _():
            sent(lsum2, l2_send.at[0])


def body(n_seq, queries, keys, values, doc_lengths, out_weight):
    rows, width = queries.shape
    kv_width = keys.shape[1]
    depth, wc = out_weight.shape
    pairs = n_seq // 2
    groups = pairs // 4
    heads = width // DH
    part = rows * 2 // CHUNKS
    wcp = min(PIECE, wc)
    pieces = wc // wcp
    slots = -(-(MOST - 1) // rows) + 1
    hbm = pl.BlockSpec(memory_space=pl.ANY)
    bf, f32, dma = jnp.bfloat16, jnp.float32, pltpu.SemaphoreType.DMA
    return pl.pallas_call(
        functools.partial(kernel, n_seq),
        out_shape=jax.ShapeDtypeStruct((rows, wc * 2 * (pairs // 4)), bf),
        in_specs=[pl.BlockSpec(memory_space=pltpu.SMEM), hbm, hbm, hbm, hbm],
        out_specs=hbm,
        scratch_shapes=[
            pltpu.VMEM((rows, width), bf),
            pltpu.VMEM((rows, wc * 2 * groups), bf),
            pltpu.VMEM((slots, 2, rows, kv_width), bf),
            pltpu.VMEM((pairs, pieces, depth, wcp), bf),
            pltpu.VMEM((rows, rows), f32),
            pltpu.VMEM((DH, rows), bf),
            pltpu.VMEM((heads, 1, rows), f32),
            pltpu.VMEM((heads, 1, rows), f32),
            pltpu.VMEM((heads, DH, rows), f32),
            pltpu.VMEM((2, 2, rows, width // 2), bf),
            pltpu.VMEM((5, pieces, CHUNKS, part, wcp), f32),
            pltpu.VMEM((groups, pieces, CHUNKS, part, wcp), f32),
            pltpu.VMEM((pairs, pieces, CHUNKS, part, wcp), bf),
            pltpu.VMEM((pairs, pieces, CHUNKS, part, wcp), bf),
            pltpu.VMEM((groups, pieces, CHUNKS // 2, part, wcp), bf),
            pltpu.VMEM((groups, pieces, CHUNKS // 2, part, wcp), bf),
            pltpu.VMEM((2, 2, rows, width // 2), bf),
            pltpu.VMEM((pieces, CHUNKS, part, wcp), bf),
            pltpu.VMEM((pieces, CHUNKS, part, wcp), bf),
            pltpu.VMEM((pieces, CHUNKS, part, wcp), bf),
            dma((4,)), dma((1,)), dma((2, 2)), dma((3, 2)), dma((slots, 2)),
            dma((pairs - 1,)), dma((pairs - 1, pieces)), dma((pairs - 1,)), dma((pairs - 1, pieces)),
            dma((2,)), dma((2,)), dma((pairs,)), dma((pairs, pieces, 2)), dma((pairs,)), dma((pairs, pieces, 2)),
            dma((groups,)), dma((groups, pieces)),
            dma((2, 2)), dma((2, 2)), dma((1,)), dma((pieces, 2)), dma((1,)), dma((pieces, CHUNKS)),
        ],
        compiler_params=pltpu.CompilerParams(
            collective_id=0, has_side_effects=True, vmem_limit_bytes=56 * 1024 * 1024
        ),
    )(doc_lengths, queries, keys, values, out_weight)


def solution(mesh):
    return jax.shard_map(
        functools.partial(body, mesh.shape["seq"]),
        mesh=mesh,
        in_specs=(P("seq", "head"), P("seq", "head"), P("seq", "head"), P(), P("head", "seq")),
        out_specs=P("seq", "head"),
        check_vma=False,
    )
```

```python
import functools
import math

import jax
import jax.numpy as jnp
from jax import lax
from jax.experimental import pallas as pl
from jax.experimental.pallas import tpu as pltpu
from jax.sharding import PartitionSpec as P

HQ = 32
KV = 8
DH = 128
MOST = 2048
CHUNKS = 4
PIECE = 128
MESH = pl.DeviceIdType.MESH


def kernel(
    n_seq, lens_ref, q_hbm, k_hbm, v_hbm, w_hbm, out_hbm,
    q_ref, out_ref, kvbuf, wbuf, bias, vt, mx, sm, acc, both,
    tmp, keep, sum1, sum2, give3, got3, lent, lsum1, lsum2, lgot,
    load_sem, out_sem, kvz_send, kvy_send, kv_recv, wl_send, wl_recv, wr_send, wr_recv,
    at_send, at_recv, s1_send, s1_recv, s2_send, s2_recv, s3_send, s3_recv,
    la_send, la_recv, l1_send, l1_recv, l2_send, l2_recv,
):
    s, h = lax.axis_index("seq"), lax.axis_index("head")
    pairs = n_seq // 2
    p, m = s // 2, lax.rem(s, 2)
    mate = s + 1 - 2 * m
    right = lax.rem(p + 1, pairs) * 2 + m
    left = lax.rem(p + pairs - 1, pairs) * 2 + m
    near = h + 1 - 2 * lax.rem(h, 2)
    far = lax.rem(h + 2, 4)
    rows = q_ref.shape[0]
    depth, wc = w_hbm.shape
    pieces, wcp = wbuf.shape[1], wbuf.shape[3]
    half = depth // 2
    groups = pairs // 4
    group_size = HQ // KV
    part = rows * 2 // CHUNKS
    wide = 2 if pieces % 2 == 0 else 1
    split = pieces // 2 if pieces % (2 * wide) == 0 else pieces
    has_up, has_down = p + 1 < pairs, p >= 1
    is_last, is_helper = p == pairs - 1, p == pairs - 2
    scale = DH ** (-0.5) * math.log2(math.e)

    def copy(src, dst, send, recv, seq, head):
        return pltpu.make_async_remote_copy(
            src_ref=src, dst_ref=dst, send_sem=send, recv_sem=recv,
            device_id={"seq": seq, "head": head}, device_id_type=MESH,
        )

    def kv_copy(src_slot, dst_slot, j, send, target):
        cols = pl.ds(pl.multiple_of(j * DH, DH), DH)
        return copy(kvbuf.at[src_slot, :, :, cols], kvbuf.at[dst_slot, :, :, cols],
                    send.at[j], kv_recv.at[dst_slot, j], target, h)

    def w_copy(block, c, step, send, recv, target):
        piece = wbuf.at[block, c]
        return copy(piece, piece, send.at[step], recv.at[step, c], target, h)

    def left_copy(step, c):
        return w_copy(jnp.minimum(p + step, pairs - 1), c, step, wl_send, wl_recv, left)

    def right_copy(step, c):
        return w_copy(jnp.maximum(p - step, 0), c, step, wr_send, wr_recv, right)

    loads = [
        pltpu.make_async_copy(k_hbm, kvbuf.at[0, 0], load_sem.at[0]),
        pltpu.make_async_copy(v_hbm, kvbuf.at[0, 1], load_sem.at[1]),
    ] + [
        pltpu.make_async_copy(w_hbm.at[:, c * wcp:(c + 1) * wcp], wbuf.at[p, c], load_sem.at[3])
        for c in range(pieces)
    ] + [pltpu.make_async_copy(q_hbm, q_ref, load_sem.at[2])]
    for load in loads:
        load.start()

    barrier = pltpu.get_barrier_semaphore()

    def greet(seq, head):
        pl.semaphore_signal(barrier, inc=1, device_id={"seq": seq, "head": head}, device_id_type=MESH)

    for seq, head in ((mate, h), (s, near), (s, far)):
        greet(seq, head)
    for there, seq in ((has_down, left), (has_up, right)):
        @pl.when(there)
        def _():
            greet(seq, h)

    @pl.when(is_last)
    def _():
        greet(left, far)

    greeted = 3 + sum(jnp.where(there, 1, 0) for there in (has_up, has_down, is_helper))
    pl.semaphore_wait(barrier, greeted)

    loads[0].wait()
    loads[1].wait()
    has_next = s + 2 < n_seq
    for j in range(2):
        @pl.when(has_next)
        def _():
            kv_copy(0, 2, j, kvz_send.at[0], right).start()

        @pl.when(m == 0)
        def _():
            kv_copy(0, 1, j, kvy_send.at[0], mate).start()

    pltpu.make_async_copy(wbuf.at[p], wbuf.at[p], load_sem.at[3]).wait()

    @pl.when(has_down)
    def _():
        for c in range(pieces):
            left_copy(0, c).start()

    q_pos = s * rows + lax.broadcasted_iota(jnp.int32, (1, rows), 1)
    start = jnp.int32(0)
    first = jnp.zeros((1, rows), jnp.int32)
    for d in range(1, lens_ref.shape[0]):
        start = start + lens_ref[d - 1]
        first = jnp.where(q_pos >= start, start, first)

    loads[-1].wait()

    def attn_copy(j):
        return copy(both.at[1, j], both.at[0, j], at_send.at[j], at_recv.at[j], mate, h)

    def lend_own(j):
        return copy(both.at[1, j], lent.at[1, j], la_send.at[0, j], la_recv.at[0, j], left, h)

    def lend_other(j, source, target):
        return copy(source, lent.at[0, j], la_send.at[1, j], la_recv.at[1, j], target, h)

    def finish(j):
        def one(g, _):
            i = j * group_size + g
            full = jnp.transpose(acc[i] / sm[i])
            both[1, j, :, pl.ds(pl.multiple_of(g * DH, DH), DH)] = full.astype(jnp.bfloat16)
            return 0

        lax.fori_loop(0, group_size, one, 0)
        @pl.when(is_last)
        def _():
            lend_own(j).start()

    def take_left(t, c):
        left_copy(t, c).wait_recv()

        @pl.when(has_down)
        def _():
            left_copy(t + 1, c).start()

    def take_right(t, c):
        right_copy(t, c).wait_recv()

        @pl.when(has_up & jnp.logical_not(is_helper & (p == t + 1)))
        def _():
            right_copy(t + 1, c).start()

    def step(i, _):
        k = jnp.maximum(i - 2, 0)
        w = lax.rem(k, 4)
        slot = jnp.where(i < 2, 0, 2 + 2 * (k // 4) - lax.rem(w, 2))
        j = jnp.where(i < 2, i, w // 2)

        @pl.when((i >= 2) & (s >= slot))
        def _():
            kv_copy(slot, slot, j, kvz_send.at[0], right).wait_recv()

            @pl.when((slot == 2) & has_next)
            def _():
                kv_copy(2, 4, j, kvz_send.at[1], right).start()

            @pl.when(slot == 2)
            def _():
                kv_copy(2, 3 - 2 * m, j, kvy_send.at[1], mate).start()

            @pl.when((slot == 4) & (m == 1))
            def _():
                kv_copy(4, 3, j, kvy_send.at[2], mate).start()

        @pl.when(i == 8)
        def _():
            attn_copy(0).start()

        @pl.when((i == 4) & has_up)
        def _():
            for c in range(split):
                right_copy(0, c).start()

            @pl.when(jnp.logical_not(is_helper))
            def _():
                for c in range(split, pieces):
                    right_copy(0, c).start()

        for c in range(pieces):
            @pl.when((i == 11 - 2 * (pieces - c)) & has_up)
            def _():
                take_left(0, c)

        @pl.when(s >= slot)
        def _():
            cols = pl.ds(pl.multiple_of(j * DH, DH), DH)
            k_pos = (s - slot) * rows + lax.broadcasted_iota(jnp.int32, (rows, rows), 0)
            bias[...] = jnp.where((k_pos >= first) & (k_pos <= q_pos), 0.0, -1e30)
            vt[...] = jnp.transpose(kvbuf[slot, 1, :, cols])

            def one(g, _):
                at = j * group_size + g
                q = q_ref[:, pl.ds(pl.multiple_of(at * DH, DH), DH)]
                scores = lax.dot_general(
                    kvbuf[slot, 0, :, cols], q, (((1,), (1,)), ((), ())),
                    preferred_element_type=jnp.float32,
                ) * scale + bias[...]
                top = jnp.max(scores, axis=0, keepdims=True)
                old = jnp.where(i < 2, jnp.full_like(top, -1e30), mx[at])
                new = jnp.maximum(old, top)
                probs = jnp.exp2(scores - new)
                fade = jnp.exp2(old - new)
                mx[at] = new
                total = jnp.sum(probs, axis=0, keepdims=True)
                sm[at] = jnp.where(i < 2, total, sm[at] * fade + total)
                mixed = jnp.dot(vt[...], probs.astype(jnp.bfloat16), preferred_element_type=jnp.float32)

                @pl.when(i < 2)
                def _():
                    acc[at] = mixed

                @pl.when(i >= 2)
                def _():
                    acc[at] = acc[at] * fade + mixed

                return 0

            lax.fori_loop(0, group_size, one, 0)

        for at, jj in ((7, 0), (9, 1)):
            @pl.when(i == at)
            def _():
                finish(jj)

        return 0

    lax.fori_loop(0, 10, step, 0)
    attn_copy(1).start()

    per_side = CHUNKS // 2

    def rows_of(side):
        return pl.ds(side * per_side, per_side)

    def first_copy(b, c, side):
        piece = sum1.at[b, c, rows_of(side)]
        return copy(piece, piece, s1_send.at[b], s1_recv.at[b, c, side], s, near)

    def second_copy(b, c, side):
        piece = sum2.at[b, c, rows_of(side)]
        return copy(piece, piece, s2_send.at[b], s2_recv.at[b, c, side], s, far)

    def third_copy(g, c):
        return copy(give3.at[g, c], got3.at[g, c], s3_send.at[g], s3_recv.at[g, c], mate, h)

    def odd(b):
        return lax.rem(b // groups + h, 2) == 1

    def product(source, b, c, n, r):
        side = r // per_side
        at = pl.multiple_of(lax.rem(r, per_side) * part, part)

        def weights(lo):
            return jnp.concatenate([wbuf[b, c + i, lo:lo + half, :] for i in range(n)], axis=1)

        y = (jnp.dot(source[side, 0, pl.ds(at, part), :], weights(0), preferred_element_type=jnp.float32)
             + jnp.dot(source[side, 1, pl.ds(at, part), :], weights(half), preferred_element_type=jnp.float32))
        return [y[:, i * wcp:(i + 1) * wcp] for i in range(n)]

    def compute(b, slot, c, n, sides):
        lo, hi = sides[0] * per_side, (sides[-1] + 1) * per_side

        @pl.when(odd(b))
        def _():
            def chunk(r, _):
                for i, y in enumerate(product(both, b, c, n, r)):
                    sum1[b, c + i, r] = y.astype(jnp.bfloat16)
                return 0

            lax.fori_loop(lo, hi, chunk, 0, unroll=True)
            for side in sides:
                for i in range(n):
                    first_copy(b, c + i, side).start()

        @pl.when(jnp.logical_not(odd(b)))
        def _():
            def chunk(r, _):
                for i, y in enumerate(product(both, b, c, n, r)):
                    tmp[slot, c + i, r] = y
                return 0

            lax.fori_loop(lo, hi, chunk, 0, unroll=True)

    def settle(b, slot, c, sides):
        @pl.when(jnp.logical_not(odd(b)))
        def _():
            home = b // groups == h
            g = lax.rem(b, groups)

            def one(side, _):
                first_copy(b, c, side).wait_recv()

                @pl.when(home)
                def _():
                    for k in range(per_side):
                        r = side * per_side + k
                        keep[g, c, r] = tmp[slot, c, r] + sum1[b, c, r].astype(jnp.float32)

                @pl.when(jnp.logical_not(home))
                def _():
                    for k in range(per_side):
                        r = side * per_side + k
                        sum2[b, c, r] = (tmp[slot, c, r] + sum1[b, c, r].astype(jnp.float32)).astype(jnp.bfloat16)
                    second_copy(b, c, side).start()

                return 0

            lax.fori_loop(sides[0], sides[-1] + 1, one, 0)

    def early_pieces(e):
        return jnp.where(is_last & (e == 2), split, pieces)

    def early_compute(e, side):
        b, exists, _, _ = block_at(e)

        @pl.when(exists)
        def _():
            def one(k, _):
                compute(b, e, k * wide, wide, (side,))
                return 0

            lax.fori_loop(0, early_pieces(e) // wide, one, 0)

    def early_settle(e, side):
        b, exists, _, _ = block_at(e)

        @pl.when(exists)
        def _():
            def one(c, _):
                settle(b, e, c, (side,))
                return 0

            lax.fori_loop(0, early_pieces(e), one, 0)

    def lent_first(c, side):
        piece = lsum1.at[c, rows_of(side)]
        return copy(piece, piece, l1_send.at[0], l1_recv.at[c, side], s, near)

    def lent_result(c, r):
        return copy(lsum2.at[c, r], lgot.at[c, r], l2_send.at[0], l2_recv.at[c, r], right, h)

    def lent_across(c, r):
        return copy(lsum2.at[c, r], sum2.at[0, c, r], l2_send.at[0], s2_recv.at[0, c, r // per_side], right, far)

    def help_step(c, side):
        at = side * per_side

        @pl.when(odd(0))
        def _():
            def chunk(r, _):
                lsum1[c, r] = product(lent, 0, c, 1, r)[0].astype(jnp.bfloat16)
                return 0

            lax.fori_loop(at, at + per_side, chunk, 0, unroll=True)
            lent_first(c, side).start()

        @pl.when(jnp.logical_not(odd(0)))
        def _():
            def chunk(r, _):
                tmp[4, c, r] = product(lent, 0, c, 1, r)[0]
                return 0

            lax.fori_loop(at, at + per_side, chunk, 0, unroll=True)

            lent_first(c, side).wait_recv()

            def add(r, _):
                lsum2[c, r] = (tmp[4, c, r] + lsum1[c, r].astype(jnp.float32)).astype(jnp.bfloat16)

                @pl.when(h == 0)
                def _():
                    lent_result(c, r).start()

                @pl.when(h != 0)
                def _():
                    lent_across(c, r).start()

                return 0

            lax.fori_loop(at, at + per_side, add, 0)

    lead = 1 if pieces > 1 else 0

    def over(one, side, lo, hi):
        def body(c, _):
            one(c, side)
            return 0

        lax.fori_loop(lo, hi, body, 0)

    def in_order(one):
        over(one, 1, 0, lead)
        over(one, 0, 0, pieces)
        over(one, 1, lead, pieces)

    def block_at(e):
        d = (e + 1) // 2
        from_up = lax.rem(e, 2) == 1
        b = jnp.where(from_up, p + d, p - d)
        return jnp.clip(b, 0, pairs - 1), (b >= 0) & (b < pairs), from_up, d

    def take_early(c):
        @pl.when(has_down & (jnp.logical_not(is_last) | (c < split)))
        def _():
            take_right(0, c)

        if c == pieces - 1:
            @pl.when(is_helper)
            def _():
                for k in range(split, pieces):
                    right_copy(0, k).start()

        @pl.when(p + 2 < pairs)
        def _():
            take_left(1, c)

    def own_side(e, _):
        for c in range(pieces):
            @pl.when(e == (c if c < min(pieces - 1, 2) else 2))
            def _():
                take_early(c)

        early_compute(e, 1)

        @pl.when(e > 0)
        def _():
            early_settle(e - 1, 1)

        return 0

    lax.fori_loop(0, 4, own_side, 0)
    early_settle(3, 1)

    for j in range(2):
        attn_copy(j).wait_recv()
        if j == 0:
            @pl.when(is_last)
            def _():
                lend_other(0, both.at[0, 0], left).start()

    late = is_last

    def other_side(k, _):
        order = (2, 1, 0, 3)

        def at(k):
            return sum(jnp.where(k == i, e, 0) for i, e in enumerate(order))

        @pl.when(jnp.logical_not(late))
        def _():
            early_compute(at(k), 0)

        @pl.when(is_helper & (k == 0))
        def _():
            for j in range(2):
                lend_own(j).wait_recv()
            lend_other(1, lent.at[1, 1], mate).start()

        @pl.when(jnp.logical_not(late) & (k > 0))
        def _():
            early_settle(at(k - 1), 0)

        return 0

    lax.fori_loop(0, 4, other_side, 0)

    @pl.when(jnp.logical_not(late))
    def _():
        early_settle(3, 0)

    def result(g, c, side, store):
        b = h * groups + g
        at = [side * per_side + k for k in range(per_side)]

        def usual():
            second_copy(b, c, side).wait_recv()
            for r in at:
                store(r, (keep[g, c, r] + sum2[b, c, r].astype(jnp.float32)).astype(jnp.bfloat16))

        if g > 0:
            usual()
            return
        helped = is_last & (h == 0)
        pl.when(jnp.logical_not(helped))(usual)

        @pl.when(helped)
        def _():
            for r in at:
                lent_result(c, r).wait_recv()
            second_copy(0, c, side).wait_recv()
            for r in at:
                store(r, (lgot[c, r].astype(jnp.float32) + sum2[0, c, r].astype(jnp.float32)).astype(jnp.bfloat16))

    def columns(g, c, member):
        return pl.ds(pl.multiple_of((2 * g + member) * wc + c * wcp, wcp), wcp)

    def place(g, c, r, member, value):
        at = pl.multiple_of(lax.rem(r, per_side) * part, part)
        out_ref[pl.ds(at, part), columns(g, c, member)] = value

    def out_copy(g, c, member):
        cols = columns(g, c, member)
        return pltpu.make_async_copy(out_ref.at[:, cols], out_hbm.at[:, cols], out_sem.at[0])

    def pass_on(c, side):
        for g in range(groups):
            def store(r, value):
                if side:
                    place(g, c, r, m, value)
                else:
                    give3[g, c, r] = value

            result(g, c, side, store)
            if side:
                out_copy(g, c, m).start()
            else:
                third_copy(g, c).start()

    def pass_both(c, _):
        pass_on(c, 0)
        pass_on(c, 1)
        return 0

    lowest, highest = h * groups, h * groups + groups - 1
    passed = (p < pairs - 2) & (lowest >= p - 1) & (highest <= p + 2)
    ready = is_helper & odd(0) & (lowest <= p - 1) & (highest >= p - 1) & (groups == 1)

    soon = is_helper & (lowest >= p) & (groups == 1)
    soon_pieces = max(pieces - 2, 0)

    @pl.when(passed)
    def _():
        lax.fori_loop(0, pieces, pass_both, 0)

    def block_step(e, _):
        b, exists, from_up, d = block_at(e)
        helped = is_last & (b == 0)
        helping = is_helper & (b == 0)

        @pl.when(exists & jnp.logical_not(helped))
        def _():
            def one(c, _):
                @pl.when(helping & (c > 0) & ready)
                def _():
                    pass_both(c - 1, 0)

                @pl.when(helping & (c == pieces - 1) & soon)
                def _():
                    lax.fori_loop(0, soon_pieces, pass_both, 0)

                @pl.when(from_up)
                def _():
                    take_left(d - 1, c)

                @pl.when(jnp.logical_not(from_up))
                def _():
                    take_right(d - 1, c)

                @pl.when(helping & (c < lead))
                def _():
                    help_step(c, 1)

                @pl.when(helping & (c == pieces - 1))
                def _():
                    for j in range(2):
                        lend_other(j, both.at[0, 0], left).wait_recv()
                    over(help_step, 0, 0, pieces)

                compute(b, 4, c, 1, (0, 1))
                settle(b, 4, c, (0, 1))

                @pl.when(helping & (c == pieces - 1))
                def _():
                    over(help_step, 1, lead, pieces)

                @pl.when(late & (e == 4) & (c == min(1, pieces - 1)))
                def _():
                    early_compute(0, 0)
                    early_compute(2, 0)
                    early_settle(0, 0)
                    early_settle(2, 0)

                return 0

            lax.fori_loop(0, pieces, one, 0)

        @pl.when(is_last & (e == 4))
        def _():
            def rest(c, _):
                take_right(0, c)
                compute(p - 1, 4, c, 1, (0, 1))
                settle(p - 1, 4, c, (0, 1))
                return 0

            lax.fori_loop(split, pieces, rest, 0)

        return 0

    lax.fori_loop(4, 2 * pairs - 1, block_step, 0)

    lent_to = is_last & (h == 0)

    @pl.when(lent_to)
    def _():
        in_order(pass_on)

    @pl.when(jnp.logical_not(lent_to | passed))
    def _():
        lax.fori_loop(jnp.where(ready, pieces - 1, jnp.where(soon, soon_pieces, 0)), pieces, pass_both, 0)

    for g in range(groups):
        def take_in(c, _):
            third_copy(g, c).wait_recv()
            for r in range(per_side):
                place(g, c, r, 1 - m, got3[g, c, r])
            out_copy(g, c, 1 - m).start()
            return 0

        lax.fori_loop(0, pieces, take_in, 0)

    for j in range(2):
        @pl.when(has_next)
        def _():
            kv_copy(0, 2, j, kvz_send.at[0], right).wait_send()

        @pl.when((s >= 2) & has_next)
        def _():
            kv_copy(2, 4, j, kvz_send.at[1], right).wait_send()

        @pl.when(m == 0)
        def _():
            kv_copy(0, 1, j, kvy_send.at[0], mate).wait_send()

        @pl.when(s >= 2)
        def _():
            kv_copy(2, 3 - 2 * m, j, kvy_send.at[1], mate).wait_send()

        @pl.when((s >= 4) & (m == 1))
        def _():
            kv_copy(4, 3, j, kvy_send.at[2], mate).wait_send()

        attn_copy(j).wait_send()

    def sent(ref, sem):
        copy(ref, ref, sem, s1_recv.at[0, 0, 0], s, near).wait_send()

    def drain(b, _):
        @pl.when(has_down & (p + b < pairs))
        def _():
            sent(wbuf.at[b], wl_send.at[b])

        @pl.when(has_up & (p - b >= 0) & jnp.logical_not(is_helper & (p == b)))
        def _():
            sent(wbuf.at[b], wr_send.at[b])

        lent_block = is_last & (b == 0)

        @pl.when(odd(b) & jnp.logical_not(lent_block))
        def _():
            sent(sum1.at[b], s1_send.at[b])

        @pl.when(jnp.logical_not(odd(b)) & (b // groups != h) & jnp.logical_not(lent_block))
        def _():
            sent(sum2.at[b], s2_send.at[b])

        return 0

    lax.fori_loop(0, pairs, drain, 0)
    for g in range(groups):
        sent(give3.at[g], s3_send.at[g])

    pltpu.make_async_copy(out_ref, out_hbm, out_sem.at[0]).wait()

    @pl.when(is_last)
    def _():
        for j in range(2):
            lend_own(j).wait_send()
        lend_other(0, both.at[0, 0], left).wait_send()

    @pl.when(is_helper)
    def _():
        lend_other(1, lent.at[1, 1], mate).wait_send()

        @pl.when(odd(0))
        def _():
            sent(lsum1, l1_send.at[0])

        @pl.when(jnp.logical_not(odd(0)))
        def _():
            sent(lsum2, l2_send.at[0])


def body(n_seq, queries, keys, values, doc_lengths, out_weight):
    rows, width = queries.shape
    kv_width = keys.shape[1]
    depth, wc = out_weight.shape
    pairs = n_seq // 2
    groups = pairs // 4
    heads = width // DH
    part = rows * 2 // CHUNKS
    wcp = min(PIECE, wc)
    pieces = wc // wcp
    slots = -(-(MOST - 1) // rows) + 1
    hbm = pl.BlockSpec(memory_space=pl.ANY)
    bf, f32, dma = jnp.bfloat16, jnp.float32, pltpu.SemaphoreType.DMA
    return pl.pallas_call(
        functools.partial(kernel, n_seq),
        out_shape=jax.ShapeDtypeStruct((rows, wc * 2 * (pairs // 4)), bf),
        in_specs=[pl.BlockSpec(memory_space=pltpu.SMEM), hbm, hbm, hbm, hbm],
        out_specs=hbm,
        scratch_shapes=[
            pltpu.VMEM((rows, width), bf),
            pltpu.VMEM((rows, wc * 2 * groups), bf),
            pltpu.VMEM((slots, 2, rows, kv_width), bf),
            pltpu.VMEM((pairs, pieces, depth, wcp), bf),
            pltpu.VMEM((rows, rows), f32),
            pltpu.VMEM((DH, rows), bf),
            pltpu.VMEM((heads, 1, rows), f32),
            pltpu.VMEM((heads, 1, rows), f32),
            pltpu.VMEM((heads, DH, rows), f32),
            pltpu.VMEM((2, 2, rows, width // 2), bf),
            pltpu.VMEM((5, pieces, CHUNKS, part, wcp), f32),
            pltpu.VMEM((groups, pieces, CHUNKS, part, wcp), f32),
            pltpu.VMEM((pairs, pieces, CHUNKS, part, wcp), bf),
            pltpu.VMEM((pairs, pieces, CHUNKS, part, wcp), bf),
            pltpu.VMEM((groups, pieces, CHUNKS // 2, part, wcp), bf),
            pltpu.VMEM((groups, pieces, CHUNKS // 2, part, wcp), bf),
            pltpu.VMEM((2, 2, rows, width // 2), bf),
            pltpu.VMEM((pieces, CHUNKS, part, wcp), bf),
            pltpu.VMEM((pieces, CHUNKS, part, wcp), bf),
            pltpu.VMEM((pieces, CHUNKS, part, wcp), bf),
            dma((4,)), dma((1,)), dma((2, 2)), dma((3, 2)), dma((slots, 2)),
            dma((pairs - 1,)), dma((pairs - 1, pieces)), dma((pairs - 1,)), dma((pairs - 1, pieces)),
            dma((2,)), dma((2,)), dma((pairs,)), dma((pairs, pieces, 2)), dma((pairs,)), dma((pairs, pieces, 2)),
            dma((groups,)), dma((groups, pieces)),
            dma((2, 2)), dma((2, 2)), dma((1,)), dma((pieces, 2)), dma((1,)), dma((pieces, CHUNKS)),
        ],
        compiler_params=pltpu.CompilerParams(
            collective_id=0, has_side_effects=True, vmem_limit_bytes=56 * 1024 * 1024
        ),
    )(doc_lengths, queries, keys, values, out_weight)


def solution(mesh):
    return jax.shard_map(
        functools.partial(body, mesh.shape["seq"]),
        mesh=mesh,
        in_specs=(P("seq", "head"), P("seq", "head"), P("seq", "head"), P(), P("head", "seq")),
        out_specs=P("seq", "head"),
        check_vma=False,
    )
```

```python
import functools
import math

import jax
import jax.numpy as jnp
from jax import lax
from jax.experimental import pallas as pl
from jax.experimental.pallas import tpu as pltpu
from jax.sharding import PartitionSpec as P

HQ = 32
KV = 8
DH = 128
MOST = 2048
CHUNKS = 4
OUT_PARTS = 4
PIECE = 128
MESH = pl.DeviceIdType.MESH


def kernel(
    n_seq, lens_ref, q_hbm, k_hbm, v_hbm, w_hbm, out_hbm,
    q_ref, out_ref, kvbuf, wbuf, bias, vt, mx, sm, acc, both,
    tmp, keep, sum1, sum2, give3, lent, lsum1, lsum2, lgot,
    load_sem, out_sem, kvz_send, kvy_send, kv_recv, wl_send, wl_recv, wr_send, wr_recv,
    at_send, at_recv, s1_send, s1_recv, s2_send, s2_recv, s3_send, s3_recv,
    la_send, la_recv, l1_send, l1_recv, l2_send, l2_recv,
):
    s, h = lax.axis_index("seq"), lax.axis_index("head")
    pairs = n_seq // 2
    p, m = s // 2, lax.rem(s, 2)
    mate = s + 1 - 2 * m
    right = lax.rem(p + 1, pairs) * 2 + m
    left = lax.rem(p + pairs - 1, pairs) * 2 + m
    near = h + 1 - 2 * lax.rem(h, 2)
    far = lax.rem(h + 2, 4)
    rows = q_ref.shape[0]
    depth, wc = w_hbm.shape
    pieces, wcp = wbuf.shape[1], wbuf.shape[3]
    half = depth // 2
    groups = pairs // 4
    group_size = HQ // KV
    part = rows * 2 // CHUNKS
    wide = 2 if pieces % 2 == 0 else 1
    split = pieces // 2 if pieces % (2 * wide) == 0 else pieces
    has_up, has_down = p + 1 < pairs, p >= 1
    is_last, is_helper = p == pairs - 1, p == pairs - 2
    scale = DH ** (-0.5) * math.log2(math.e)

    def copy(src, dst, send, recv, seq, head):
        return pltpu.make_async_remote_copy(
            src_ref=src, dst_ref=dst, send_sem=send, recv_sem=recv,
            device_id={"seq": seq, "head": head}, device_id_type=MESH,
        )

    def kv_copy(src_slot, dst_slot, j, send, target):
        cols = pl.ds(pl.multiple_of(j * DH, DH), DH)
        return copy(kvbuf.at[src_slot, :, :, cols], kvbuf.at[dst_slot, :, :, cols],
                    send.at[j], kv_recv.at[dst_slot, j], target, h)

    def w_copy(block, c, step, send, recv, target):
        piece = wbuf.at[block, c]
        return copy(piece, piece, send.at[step], recv.at[step, c], target, h)

    def left_copy(step, c):
        return w_copy(jnp.minimum(p + step, pairs - 1), c, step, wl_send, wl_recv, left)

    def right_copy(step, c):
        return w_copy(jnp.maximum(p - step, 0), c, step, wr_send, wr_recv, right)

    loads = [
        pltpu.make_async_copy(k_hbm, kvbuf.at[0, 0], load_sem.at[0]),
        pltpu.make_async_copy(v_hbm, kvbuf.at[0, 1], load_sem.at[1]),
    ] + [
        pltpu.make_async_copy(w_hbm.at[:, c * wcp:(c + 1) * wcp], wbuf.at[p, c], load_sem.at[3])
        for c in range(pieces)
    ] + [pltpu.make_async_copy(q_hbm, q_ref, load_sem.at[2])]
    for load in loads:
        load.start()

    barrier = pltpu.get_barrier_semaphore()

    def greet(seq, head):
        pl.semaphore_signal(barrier, inc=1, device_id={"seq": seq, "head": head}, device_id_type=MESH)

    for seq, head in ((mate, h), (s, near), (s, far)):
        greet(seq, head)
    for there, seq in ((has_down, left), (has_up, right)):
        @pl.when(there)
        def _():
            greet(seq, h)

    @pl.when(is_last)
    def _():
        greet(left, far)

    greeted = 3 + sum(jnp.where(there, 1, 0) for there in (has_up, has_down, is_helper))
    pl.semaphore_wait(barrier, greeted)

    loads[0].wait()
    loads[1].wait()
    has_next = s + 2 < n_seq
    for j in range(2):
        @pl.when(has_next)
        def _():
            kv_copy(0, 2, j, kvz_send.at[0], right).start()

        @pl.when(m == 0)
        def _():
            kv_copy(0, 1, j, kvy_send.at[0], mate).start()

    pltpu.make_async_copy(wbuf.at[p], wbuf.at[p], load_sem.at[3]).wait()

    @pl.when(has_down)
    def _():
        for c in range(pieces):
            left_copy(0, c).start()

    q_pos = s * rows + lax.broadcasted_iota(jnp.int32, (1, rows), 1)
    start = jnp.int32(0)
    first = jnp.zeros((1, rows), jnp.int32)
    for d in range(1, lens_ref.shape[0]):
        start = start + lens_ref[d - 1]
        first = jnp.where(q_pos >= start, start, first)

    loads[-1].wait()

    def attn_copy(j):
        return copy(both.at[1, j], both.at[0, j], at_send.at[j], at_recv.at[j], mate, h)

    def lend_own(j):
        return copy(both.at[1, j], lent.at[1, j], la_send.at[0, j], la_recv.at[0, j], left, h)

    def lend_other(j, source, target):
        return copy(source, lent.at[0, j], la_send.at[1, j], la_recv.at[1, j], target, h)

    def finish(j):
        def one(g, _):
            i = j * group_size + g
            full = jnp.transpose(acc[i] / sm[i])
            both[1, j, :, pl.ds(pl.multiple_of(g * DH, DH), DH)] = full.astype(jnp.bfloat16)
            return 0

        lax.fori_loop(0, group_size, one, 0)
        @pl.when(is_last)
        def _():
            lend_own(j).start()

    def take_left(t, c):
        left_copy(t, c).wait_recv()

        @pl.when(has_down)
        def _():
            left_copy(t + 1, c).start()

    def take_right(t, c):
        right_copy(t, c).wait_recv()

        @pl.when(has_up & jnp.logical_not(is_helper & (p == t + 1)))
        def _():
            right_copy(t + 1, c).start()

    def step(i, _):
        k = jnp.maximum(i - 2, 0)
        w = lax.rem(k, 4)
        slot = jnp.where(i < 2, 0, 2 + 2 * (k // 4) - lax.rem(w, 2))
        j = jnp.where(i < 2, i, w // 2)

        @pl.when((i >= 2) & (s >= slot))
        def _():
            kv_copy(slot, slot, j, kvz_send.at[0], right).wait_recv()

            @pl.when((slot == 2) & has_next)
            def _():
                kv_copy(2, 4, j, kvz_send.at[1], right).start()

            @pl.when(slot == 2)
            def _():
                kv_copy(2, 3 - 2 * m, j, kvy_send.at[1], mate).start()

            @pl.when((slot == 4) & (m == 1))
            def _():
                kv_copy(4, 3, j, kvy_send.at[2], mate).start()

        @pl.when(i == 8)
        def _():
            attn_copy(0).start()

        @pl.when((i == 4) & has_up)
        def _():
            for c in range(split):
                right_copy(0, c).start()

            @pl.when(jnp.logical_not(is_helper))
            def _():
                for c in range(split, pieces):
                    right_copy(0, c).start()

        for c in range(pieces):
            @pl.when((i == 11 - 2 * (pieces - c)) & has_up)
            def _():
                take_left(0, c)

        @pl.when(s >= slot)
        def _():
            cols = pl.ds(pl.multiple_of(j * DH, DH), DH)
            k_pos = (s - slot) * rows + lax.broadcasted_iota(jnp.int32, (rows, rows), 0)
            bias[...] = jnp.where((k_pos >= first) & (k_pos <= q_pos), 0.0, -1e30)
            vt[...] = jnp.transpose(kvbuf[slot, 1, :, cols])

            def one(g, _):
                at = j * group_size + g
                q = q_ref[:, pl.ds(pl.multiple_of(at * DH, DH), DH)]
                scores = lax.dot_general(
                    kvbuf[slot, 0, :, cols], q, (((1,), (1,)), ((), ())),
                    preferred_element_type=jnp.float32,
                ) * scale + bias[...]
                top = jnp.max(scores, axis=0, keepdims=True)
                old = jnp.where(i < 2, jnp.full_like(top, -1e30), mx[at])
                new = jnp.maximum(old, top)
                probs = jnp.exp2(scores - new)
                fade = jnp.exp2(old - new)
                mx[at] = new
                total = jnp.sum(probs, axis=0, keepdims=True)
                sm[at] = jnp.where(i < 2, total, sm[at] * fade + total)
                mixed = jnp.dot(vt[...], probs.astype(jnp.bfloat16), preferred_element_type=jnp.float32)

                @pl.when(i < 2)
                def _():
                    acc[at] = mixed

                @pl.when(i >= 2)
                def _():
                    acc[at] = acc[at] * fade + mixed

                return 0

            lax.fori_loop(0, group_size, one, 0)

        for at, jj in ((7, 0), (9, 1)):
            @pl.when(i == at)
            def _():
                finish(jj)

        return 0

    lax.fori_loop(0, 10, step, 0)
    attn_copy(1).start()

    per_side = CHUNKS // 2

    def rows_of(side):
        return pl.ds(side * per_side, per_side)

    def first_copy(b, c, side):
        piece = sum1.at[b, c, rows_of(side)]
        return copy(piece, piece, s1_send.at[b], s1_recv.at[b, c, side], s, near)

    def second_copy(b, c, side):
        piece = sum2.at[b, c, rows_of(side)]
        return copy(piece, piece, s2_send.at[b], s2_recv.at[b, c, side], s, far)

    def columns(g, c, member):
        return pl.ds(pl.multiple_of((2 * g + member) * wc + c * wcp, wcp), wcp)

    def third_copy(g, c):
        return copy(give3.at[g, c], out_ref.at[:, columns(g, c, m)], s3_send.at[g], s3_recv.at[g, c], mate, h)

    def odd(b):
        return lax.rem(b // groups + h, 2) == 1

    def product(source, b, c, n, r):
        side = r // per_side
        at = pl.multiple_of(lax.rem(r, per_side) * part, part)

        def weights(lo):
            return jnp.concatenate([wbuf[b, c + i, lo:lo + half, :] for i in range(n)], axis=1)

        y = (jnp.dot(source[side, 0, pl.ds(at, part), :], weights(0), preferred_element_type=jnp.float32)
             + jnp.dot(source[side, 1, pl.ds(at, part), :], weights(half), preferred_element_type=jnp.float32))
        return [y[:, i * wcp:(i + 1) * wcp] for i in range(n)]

    def compute(b, slot, c, n, sides):
        lo, hi = sides[0] * per_side, (sides[-1] + 1) * per_side

        @pl.when(odd(b))
        def _():
            def chunk(r, _):
                for i, y in enumerate(product(both, b, c, n, r)):
                    sum1[b, c + i, r] = y.astype(jnp.bfloat16)
                return 0

            lax.fori_loop(lo, hi, chunk, 0, unroll=True)
            for side in sides:
                for i in range(n):
                    first_copy(b, c + i, side).start()

        @pl.when(jnp.logical_not(odd(b)))
        def _():
            def chunk(r, _):
                for i, y in enumerate(product(both, b, c, n, r)):
                    tmp[slot, c + i, r] = y
                return 0

            lax.fori_loop(lo, hi, chunk, 0, unroll=True)

    def settle(b, slot, c, sides):
        @pl.when(jnp.logical_not(odd(b)))
        def _():
            home = b // groups == h
            g = lax.rem(b, groups)

            def one(side, _):
                first_copy(b, c, side).wait_recv()

                @pl.when(home)
                def _():
                    for k in range(per_side):
                        r = side * per_side + k
                        keep[g, c, r] = tmp[slot, c, r] + sum1[b, c, r].astype(jnp.float32)

                @pl.when(jnp.logical_not(home))
                def _():
                    for k in range(per_side):
                        r = side * per_side + k
                        sum2[b, c, r] = (tmp[slot, c, r] + sum1[b, c, r].astype(jnp.float32)).astype(jnp.bfloat16)
                    second_copy(b, c, side).start()

                return 0

            lax.fori_loop(sides[0], sides[-1] + 1, one, 0)

    def early_pieces(e):
        return jnp.where(is_last & (e == 2), split, pieces)

    def early_compute(e, side):
        b, exists, _, _ = block_at(e)

        @pl.when(exists)
        def _():
            def one(k, _):
                compute(b, e, k * wide, wide, (side,))
                return 0

            lax.fori_loop(0, early_pieces(e) // wide, one, 0)

    def early_settle(e, side):
        b, exists, _, _ = block_at(e)

        @pl.when(exists)
        def _():
            def one(c, _):
                settle(b, e, c, (side,))
                return 0

            lax.fori_loop(0, early_pieces(e), one, 0)

    def lent_first(c, side):
        piece = lsum1.at[c, rows_of(side)]
        return copy(piece, piece, l1_send.at[0], l1_recv.at[c, side], s, near)

    def lent_result(c, r):
        return copy(lsum2.at[c, r], lgot.at[c, r], l2_send.at[0], l2_recv.at[c, r], right, h)

    def lent_across(c, r):
        return copy(lsum2.at[c, r], sum2.at[0, c, r], l2_send.at[0], s2_recv.at[0, c, r // per_side], right, far)

    def help_step(c, side):
        at = side * per_side

        @pl.when(odd(0))
        def _():
            def chunk(r, _):
                lsum1[c, r] = product(lent, 0, c, 1, r)[0].astype(jnp.bfloat16)
                return 0

            lax.fori_loop(at, at + per_side, chunk, 0, unroll=True)
            lent_first(c, side).start()

        @pl.when(jnp.logical_not(odd(0)))
        def _():
            def chunk(r, _):
                tmp[4, c, r] = product(lent, 0, c, 1, r)[0]
                return 0

            lax.fori_loop(at, at + per_side, chunk, 0, unroll=True)

            lent_first(c, side).wait_recv()

            def add(r, _):
                lsum2[c, r] = (tmp[4, c, r] + lsum1[c, r].astype(jnp.float32)).astype(jnp.bfloat16)

                @pl.when(h == 0)
                def _():
                    lent_result(c, r).start()

                @pl.when(h != 0)
                def _():
                    lent_across(c, r).start()

                return 0

            lax.fori_loop(at, at + per_side, add, 0)

    lead = 1 if pieces > 1 else 0

    def over(one, side, lo, hi):
        def body(c, _):
            one(c, side)
            return 0

        lax.fori_loop(lo, hi, body, 0)

    def in_order(one):
        over(one, 1, 0, lead)
        over(one, 0, 0, pieces)
        over(one, 1, lead, pieces)

    def block_at(e):
        d = (e + 1) // 2
        from_up = lax.rem(e, 2) == 1
        b = jnp.where(from_up, p + d, p - d)
        return jnp.clip(b, 0, pairs - 1), (b >= 0) & (b < pairs), from_up, d

    def take_early(c):
        @pl.when(has_down & (jnp.logical_not(is_last) | (c < split)))
        def _():
            take_right(0, c)

        if c == pieces - 1:
            @pl.when(is_helper)
            def _():
                for k in range(split, pieces):
                    right_copy(0, k).start()

        @pl.when(p + 2 < pairs)
        def _():
            take_left(1, c)

    def own_side(e, _):
        for c in range(pieces):
            @pl.when(e == (c if c < min(pieces - 1, 2) else 2))
            def _():
                take_early(c)

        early_compute(e, 1)

        @pl.when(e > 0)
        def _():
            early_settle(e - 1, 1)

        return 0

    lax.fori_loop(0, 4, own_side, 0)
    early_settle(3, 1)

    for j in range(2):
        attn_copy(j).wait_recv()
        if j == 0:
            @pl.when(is_last)
            def _():
                lend_other(0, both.at[0, 0], left).start()

    late = is_last

    def other_side(k, _):
        order = (2, 1, 0, 3)

        def at(k):
            return sum(jnp.where(k == i, e, 0) for i, e in enumerate(order))

        @pl.when(jnp.logical_not(late))
        def _():
            early_compute(at(k), 0)

        @pl.when(is_helper & (k == 0))
        def _():
            for j in range(2):
                lend_own(j).wait_recv()
            lend_other(1, lent.at[1, 1], mate).start()

        @pl.when(jnp.logical_not(late) & (k > 0))
        def _():
            early_settle(at(k - 1), 0)

        return 0

    lax.fori_loop(0, 4, other_side, 0)

    @pl.when(jnp.logical_not(late))
    def _():
        early_settle(3, 0)

    def result(g, c, side, store):
        b = h * groups + g
        at = [side * per_side + k for k in range(per_side)]

        def usual():
            second_copy(b, c, side).wait_recv()
            for r in at:
                store(r, (keep[g, c, r] + sum2[b, c, r].astype(jnp.float32)).astype(jnp.bfloat16))

        if g > 0:
            usual()
            return
        helped = is_last & (h == 0)
        pl.when(jnp.logical_not(helped))(usual)

        @pl.when(helped)
        def _():
            for r in at:
                lent_result(c, r).wait_recv()
            second_copy(0, c, side).wait_recv()
            for r in at:
                store(r, (lgot[c, r].astype(jnp.float32) + sum2[0, c, r].astype(jnp.float32)).astype(jnp.bfloat16))

    def place(g, c, r, member, value):
        at = pl.multiple_of(lax.rem(r, per_side) * part, part)
        out_ref[pl.ds(at, part), columns(g, c, member)] = value

    def out_copy(g, c, member):
        cols = columns(g, c, member)
        return pltpu.make_async_copy(out_ref.at[:, cols], out_hbm.at[:, cols], out_sem.at[0])

    def pass_on(c, side):
        for g in range(groups):
            def store(r, value):
                if side:
                    place(g, c, r, m, value)
                else:
                    give3[g, c, pl.ds(r * part, part), :] = value

            result(g, c, side, store)
            if side:
                out_copy(g, c, m).start()
            else:
                third_copy(g, c).start()

    def pass_both(c, _):
        pass_on(c, 0)
        pass_on(c, 1)
        return 0

    lowest, highest = h * groups, h * groups + groups - 1
    passed = (p < pairs - 2) & (lowest >= p - 1) & (highest <= p + 2)
    ready = is_helper & odd(0) & (lowest <= p - 1) & (highest >= p - 1) & (groups == 1)

    soon = is_helper & (lowest >= p) & (groups == 1)
    soon_pieces = max(pieces - 2, 0)

    @pl.when(passed)
    def _():
        lax.fori_loop(0, pieces, pass_both, 0)

    def block_step(e, _):
        b, exists, from_up, d = block_at(e)
        helped = is_last & (b == 0)
        helping = is_helper & (b == 0)

        @pl.when(exists & jnp.logical_not(helped))
        def _():
            def one(c, _):
                @pl.when(helping & (c > 0) & ready)
                def _():
                    pass_both(c - 1, 0)

                @pl.when(helping & (c == pieces - 1) & soon)
                def _():
                    lax.fori_loop(0, soon_pieces, pass_both, 0)

                @pl.when(from_up)
                def _():
                    take_left(d - 1, c)

                @pl.when(jnp.logical_not(from_up))
                def _():
                    take_right(d - 1, c)

                @pl.when(helping & (c < lead))
                def _():
                    help_step(c, 1)

                @pl.when(helping & (c == pieces - 1))
                def _():
                    for j in range(2):
                        lend_other(j, both.at[0, 0], left).wait_recv()
                    over(help_step, 0, 0, pieces)

                compute(b, 4, c, 1, (0, 1))
                settle(b, 4, c, (0, 1))

                @pl.when(helping & (c == pieces - 1))
                def _():
                    over(help_step, 1, lead, pieces)

                @pl.when(late & (e == 4) & (c == min(1, pieces - 1)))
                def _():
                    early_compute(0, 0)
                    early_compute(2, 0)
                    early_settle(0, 0)
                    early_settle(2, 0)

                return 0

            lax.fori_loop(0, pieces, one, 0)

        @pl.when(is_last & (e == 4))
        def _():
            def rest(c, _):
                take_right(0, c)
                compute(p - 1, 4, c, 1, (0, 1))
                settle(p - 1, 4, c, (0, 1))
                return 0

            lax.fori_loop(split, pieces, rest, 0)

        return 0

    lax.fori_loop(4, 2 * pairs - 1, block_step, 0)

    lent_to = is_last & (h == 0)

    @pl.when(lent_to)
    def _():
        in_order(pass_on)

    @pl.when(jnp.logical_not(lent_to | passed))
    def _():
        lax.fori_loop(jnp.where(ready, pieces - 1, jnp.where(soon, soon_pieces, 0)), pieces, pass_both, 0)

    for g in range(groups):
        def take_in(c, _):
            third_copy(g, c).wait_recv()
            out_copy(g, c, 1 - m).start()
            return 0

        lax.fori_loop(0, pieces, take_in, 0)

    for j in range(2):
        @pl.when(has_next)
        def _():
            kv_copy(0, 2, j, kvz_send.at[0], right).wait_send()

        @pl.when((s >= 2) & has_next)
        def _():
            kv_copy(2, 4, j, kvz_send.at[1], right).wait_send()

        @pl.when(m == 0)
        def _():
            kv_copy(0, 1, j, kvy_send.at[0], mate).wait_send()

        @pl.when(s >= 2)
        def _():
            kv_copy(2, 3 - 2 * m, j, kvy_send.at[1], mate).wait_send()

        @pl.when((s >= 4) & (m == 1))
        def _():
            kv_copy(4, 3, j, kvy_send.at[2], mate).wait_send()

        attn_copy(j).wait_send()

    def sent(ref, sem):
        copy(ref, ref, sem, s1_recv.at[0, 0, 0], s, near).wait_send()

    def drain(b, _):
        @pl.when(has_down & (p + b < pairs))
        def _():
            sent(wbuf.at[b], wl_send.at[b])

        @pl.when(has_up & (p - b >= 0) & jnp.logical_not(is_helper & (p == b)))
        def _():
            sent(wbuf.at[b], wr_send.at[b])

        lent_block = is_last & (b == 0)

        @pl.when(odd(b) & jnp.logical_not(lent_block))
        def _():
            sent(sum1.at[b], s1_send.at[b])

        @pl.when(jnp.logical_not(odd(b)) & (b // groups != h) & jnp.logical_not(lent_block))
        def _():
            sent(sum2.at[b], s2_send.at[b])

        return 0

    lax.fori_loop(0, pairs, drain, 0)
    for g in range(groups):
        sent(give3.at[g], s3_send.at[g])

    pltpu.make_async_copy(out_ref, out_hbm, out_sem.at[0]).wait()

    @pl.when(is_last)
    def _():
        for j in range(2):
            lend_own(j).wait_send()
        lend_other(0, both.at[0, 0], left).wait_send()

    @pl.when(is_helper)
    def _():
        lend_other(1, lent.at[1, 1], mate).wait_send()

        @pl.when(odd(0))
        def _():
            sent(lsum1, l1_send.at[0])

        @pl.when(jnp.logical_not(odd(0)))
        def _():
            sent(lsum2, l2_send.at[0])


def hand_over(src, dst, buf, sem):
    part = src.shape[0] // OUT_PARTS
    rows = [pl.ds(i * part, part) for i in range(OUT_PARTS)]
    ins = [pltpu.make_async_copy(src.at[r], buf.at[r], sem.at[0, i]) for i, r in enumerate(rows)]
    outs = [pltpu.make_async_copy(buf.at[r], dst.at[r], sem.at[1, i]) for i, r in enumerate(rows)]
    for load in ins:
        load.start()
    for load, store in zip(ins, outs):
        load.wait()
        store.start()
    for store in outs:
        store.wait()


def body(n_seq, queries, keys, values, doc_lengths, out_weight):
    rows, width = queries.shape
    kv_width = keys.shape[1]
    depth, wc = out_weight.shape
    pairs = n_seq // 2
    groups = pairs // 4
    heads = width // DH
    part = rows * 2 // CHUNKS
    wcp = min(PIECE, wc)
    pieces = wc // wcp
    slots = -(-(MOST - 1) // rows) + 1
    hbm = pl.BlockSpec(memory_space=pl.ANY)
    bf, f32, dma = jnp.bfloat16, jnp.float32, pltpu.SemaphoreType.DMA
    mixed = pl.pallas_call(
        functools.partial(kernel, n_seq),
        out_shape=jax.ShapeDtypeStruct((rows, wc * 2 * (pairs // 4)), bf),
        in_specs=[pl.BlockSpec(memory_space=pltpu.SMEM), hbm, hbm, hbm, hbm],
        out_specs=hbm,
        scratch_shapes=[
            pltpu.VMEM((rows, width), bf),
            pltpu.VMEM((rows, wc * 2 * groups), bf),
            pltpu.VMEM((slots, 2, rows, kv_width), bf),
            pltpu.VMEM((pairs, pieces, depth, wcp), bf),
            pltpu.VMEM((rows, rows), f32),
            pltpu.VMEM((DH, rows), bf),
            pltpu.VMEM((heads, 1, rows), f32),
            pltpu.VMEM((heads, 1, rows), f32),
            pltpu.VMEM((heads, DH, rows), f32),
            pltpu.VMEM((2, 2, rows, width // 2), bf),
            pltpu.VMEM((5, pieces, CHUNKS, part, wcp), f32),
            pltpu.VMEM((groups, pieces, CHUNKS, part, wcp), f32),
            pltpu.VMEM((pairs, pieces, CHUNKS, part, wcp), bf),
            pltpu.VMEM((pairs, pieces, CHUNKS, part, wcp), bf),
            pltpu.VMEM((groups, pieces, rows, wcp), bf),
            pltpu.VMEM((2, 2, rows, width // 2), bf),
            pltpu.VMEM((pieces, CHUNKS, part, wcp), bf),
            pltpu.VMEM((pieces, CHUNKS, part, wcp), bf),
            pltpu.VMEM((pieces, CHUNKS, part, wcp), bf),
            dma((4,)), dma((1,)), dma((2, 2)), dma((3, 2)), dma((slots, 2)),
            dma((pairs - 1,)), dma((pairs - 1, pieces)), dma((pairs - 1,)), dma((pairs - 1, pieces)),
            dma((2,)), dma((2,)), dma((pairs,)), dma((pairs, pieces, 2)), dma((pairs,)), dma((pairs, pieces, 2)),
            dma((groups,)), dma((groups, pieces)),
            dma((2, 2)), dma((2, 2)), dma((1,)), dma((pieces, 2)), dma((1,)), dma((pieces, CHUNKS)),
        ],
        compiler_params=pltpu.CompilerParams(
            collective_id=0, has_side_effects=True, vmem_limit_bytes=56 * 1024 * 1024
        ),
    )(doc_lengths, queries, keys, values, out_weight)
    return pl.pallas_call(
        hand_over,
        out_shape=jax.ShapeDtypeStruct(mixed.shape, mixed.dtype),
        in_specs=[hbm],
        out_specs=hbm,
        scratch_shapes=[pltpu.VMEM(mixed.shape, mixed.dtype), dma((2, OUT_PARTS))],
        compiler_params=pltpu.CompilerParams(vmem_limit_bytes=56 * 1024 * 1024),
    )(mixed)


def solution(mesh):
    return jax.shard_map(
        functools.partial(body, mesh.shape["seq"]),
        mesh=mesh,
        in_specs=(P("seq", "head"), P("seq", "head"), P("seq", "head"), P(), P("head", "seq")),
        out_specs=P("seq", "head"),
        check_vma=False,
    )
```
